16 devices in a mesh: dp: 2 (over y, z), fsdp: 8 (over x, core).
Axes of the slice: x: 4, y: 2, z: 1, core: 2. Of those that a mesh axis runs over, the one named last changes fastest.
The devices are a block of a 4x4x8 slice.
Arguments:
- tokens: bfloat16 [32, 256, 2048], P(('dp', 'fsdp')), parts along dimension 0
- w_query: bfloat16 [2, 2048, 2048], P(None, 'fsdp')
- w_key: bfloat16 [2, 2048, 2048], P(None, 'fsdp')
- w_value: bfloat16 [2, 2048, 2048], P(None, 'fsdp')
- w_out: bfloat16 [2, 2048, 2048], P(None, 'fsdp')
- w_gate: bfloat16 [2, 2048, 8192], P(None, 'fsdp')
- w_up: bfloat16 [2, 2048, 8192], P(None, 'fsdp')
- w_down: bfloat16 [2, 8192, 2048], P(None, 'fsdp')
- g_query: bfloat16 [2, 2048], P(None, 'fsdp')
- g_key: bfloat16 [2, 2048], P(None, 'fsdp')
- g_attn: bfloat16 [2, 2048], P(None, 'fsdp')
- g_mlp: bfloat16 [2, 2048], P(None, 'fsdp')
Outputs:
- output: bfloat16 [32, 256, 2048], P(('dp', 'fsdp')), parts along dimension 0
There are 2 independent parts. The reference program is written for one: setup_inputs(seed, part) draws one part's arguments, and reference() takes and returns one part's arrays. A program takes and returns all parts, laid end to end along the dimension named above; an argument that names none is the same for every part.
All inputs are finite; a program needn't handle non-finite values.
Results may differ from the reference program's by a relative error of at most 0.02.
Values are sent between devices in bfloat16 or wider.
A program may use at most 768 MiB of HBM per device.

```python
import jax
import jax.numpy as jnp
from jax import lax

D = 2048
FF = 8192
HEADS = 16
SEQ = 256
BATCH = 16
LAYERS = 2
HEAD = D // HEADS
Q_BLOCK = min(SEQ, 256)
EPS = 1e-6
THETA = 500000.0


def setup_inputs(seed: int = 0, part: int = 0) -> dict:
    key_main = jax.random.key(seed)
    key_tok = jax.random.fold_in(jax.random.key(seed + 1), part)
    key_list = jax.random.split(key_main, 11)

    def make_weight(key_w, n_rows, n_cols):
        draw = jax.random.normal(key_w, (LAYERS, n_rows, n_cols), jnp.float32)
        return (draw * n_rows ** -0.5).astype(jnp.bfloat16)

    def make_gain(key_g):
        key_mag, key_sign = jax.random.split(key_g)
        magnitude = jax.random.uniform(key_mag, (LAYERS, D), jnp.float32, 0.5, 1.5)
        sign_vec = jnp.where(jax.random.bernoulli(key_sign, 0.5, (LAYERS, D)), 1.0, -1.0)
        return (magnitude * sign_vec).astype(jnp.bfloat16)

    tokens = jax.random.normal(key_tok, (BATCH, SEQ, D), jnp.float32).astype(jnp.bfloat16)
    return dict(
        tokens=tokens,
        w_query=make_weight(key_list[0], D, D),
        w_key=make_weight(key_list[1], D, D),
        w_value=make_weight(key_list[2], D, D),
        w_out=make_weight(key_list[3], D, D),
        w_gate=make_weight(key_list[4], D, FF),
        w_up=make_weight(key_list[5], D, FF),
        w_down=make_weight(key_list[6], FF, D),
        g_query=make_gain(key_list[7]),
        g_key=make_gain(key_list[8]),
        g_attn=make_gain(key_list[9]),
        g_mlp=make_gain(key_list[10]),
    )


def rms_norm(values, gain_vec):
    mean_sq = jnp.mean(values * values, axis=-1, keepdims=True)
    return values * lax.rsqrt(mean_sq + EPS) * gain_vec.astype(jnp.float32)


def rope_tables():
    positions = jnp.arange(SEQ, dtype=jnp.float32)
    inv_freq = THETA ** (-2.0 * jnp.arange(HEAD // 2, dtype=jnp.float32) / HEAD)
    angles = positions[:, None] * inv_freq[None, :]
    return jnp.cos(angles), jnp.sin(angles)


def apply_rope(values, cos_tab, sin_tab):
    half_dim = values.shape[-1] // 2
    first = values[..., :half_dim]
    second = values[..., half_dim:]
    cos_b = cos_tab[:, None, :]
    sin_b = sin_tab[:, None, :]
    return jnp.concatenate([first * cos_b - second * sin_b, second * cos_b + first * sin_b], axis=-1)


def matmul_bf16(left, right):
    return jnp.dot(left, right, preferred_element_type=jnp.float32).astype(jnp.bfloat16)


def layer_seq(seq_x, layer_w, cos_tab, sin_tab):
    w_query, w_key, w_value, w_out, w_gate, w_up, w_down, g_query, g_key, g_attn, g_mlp = layer_w
    q_lin = matmul_bf16(seq_x, w_query)
    k_lin = matmul_bf16(seq_x, w_key)
    v_lin = matmul_bf16(seq_x, w_value)
    q_rot = apply_rope(rms_norm(q_lin.astype(jnp.float32), g_query).reshape(SEQ, HEADS, HEAD), cos_tab, sin_tab).astype(jnp.bfloat16)
    k_rot = apply_rope(rms_norm(k_lin.astype(jnp.float32), g_key).reshape(SEQ, HEADS, HEAD), cos_tab, sin_tab).astype(jnp.bfloat16)
    k_full = k_rot.astype(jnp.float32)
    v_full = v_lin.reshape(SEQ, HEADS, HEAD).astype(jnp.float32)
    q_blocks = q_rot.reshape(SEQ // Q_BLOCK, Q_BLOCK, HEADS, HEAD)
    key_pos = jnp.arange(SEQ)

    def attend(block_in):
        q_blk, block_idx = block_in
        scores = jnp.einsum('qhd,khd->hqk', q_blk.astype(jnp.float32), k_full) * HEAD ** -0.5
        q_pos = block_idx * Q_BLOCK + jnp.arange(Q_BLOCK)
        causal = q_pos[:, None] >= key_pos[None, :]
        scores = jnp.where(causal[None, :, :], scores, -jnp.inf)
        probs = jax.nn.softmax(scores, axis=-1).astype(jnp.bfloat16).astype(jnp.float32)
        return jnp.einsum('hqk,khd->qhd', probs, v_full).astype(jnp.bfloat16)

    attn_blocks = lax.map(attend, (q_blocks, jnp.arange(SEQ // Q_BLOCK)))
    a_lin = matmul_bf16(attn_blocks.reshape(SEQ, D), w_out)
    hidden = (seq_x.astype(jnp.float32) + rms_norm(a_lin.astype(jnp.float32), g_attn)).astype(jnp.bfloat16)
    gate_proj = matmul_bf16(hidden, w_gate)
    up_proj = matmul_bf16(hidden, w_up)
    gated = (jax.nn.silu(gate_proj.astype(jnp.float32)) * up_proj.astype(jnp.float32)).astype(jnp.bfloat16)
    down_proj = matmul_bf16(gated, w_down)
    return (hidden.astype(jnp.float32) + rms_norm(down_proj.astype(jnp.float32), g_mlp)).astype(jnp.bfloat16)


def reference(tokens, w_query, w_key, w_value, w_out, w_gate, w_up, w_down, g_query, g_key, g_attn, g_mlp):
    cos_tab, sin_tab = rope_tables()

    def one_layer(carry, layer_w):
        out_seq = lax.map(lambda seq_x: layer_seq(seq_x, layer_w, cos_tab, sin_tab), carry)
        return out_seq, None

    result, _ = lax.scan(one_layer, tokens, (w_query, w_key, w_value, w_out, w_gate, w_up, w_down, g_query, g_key, g_attn, g_mlp))
    return result
```

```python
import jax
import jax.numpy as jnp
from jax import lax
from jax.sharding import PartitionSpec as P

HEAD_DIM = 128
EPS = 1e-6
THETA = 500000.0


def rope_tables(seq_len):
    positions = jnp.arange(seq_len, dtype=jnp.float32)
    inv_freq = THETA ** (-2.0 * jnp.arange(HEAD_DIM // 2, dtype=jnp.float32) / HEAD_DIM)
    angles = positions[:, None] * inv_freq[None, :]
    return jnp.cos(angles), jnp.sin(angles)


def apply_rope(values, cos_tab, sin_tab):
    half_dim = values.shape[-1] // 2
    first = values[..., :half_dim]
    second = values[..., half_dim:]
    cos_b = cos_tab[:, None, :]
    sin_b = sin_tab[:, None, :]
    return jnp.concatenate([first * cos_b - second * sin_b, second * cos_b + first * sin_b], axis=-1)


def dot_f32(left, right):
    return jnp.dot(left, right, preferred_element_type=jnp.float32)


def dot_bf16(left, right):
    return dot_f32(left, right).astype(jnp.bfloat16)


def causal_attention(q_rot, k_rot, v_heads):
    seq_len = q_rot.shape[1]
    scores = jnp.einsum('bqhd,bkhd->bhqk', q_rot, k_rot, preferred_element_type=jnp.float32) * HEAD_DIM ** -0.5
    pos = jnp.arange(seq_len)
    scores = jnp.where(pos[:, None] >= pos[None, :], scores, -jnp.inf)
    probs = jax.nn.softmax(scores, axis=-1).astype(jnp.bfloat16)
    return jnp.einsum('bhqk,bkhd->bqhd', probs, v_heads, preferred_element_type=jnp.float32).astype(jnp.bfloat16)


def residual_norm(res, lin, gain):
    lin = lin.astype(jnp.bfloat16).astype(jnp.float32)
    mean_sq = jnp.mean(lin * lin, axis=-1, keepdims=True)
    return (res.astype(jnp.float32) + lin * lax.rsqrt(mean_sq + EPS) * gain).astype(jnp.bfloat16)


def solution(mesh):
    n_dp = mesh.shape['dp']
    n_fsdp = mesh.shape['fsdp']
    pairs = [(g, g ^ 1) for g in range(n_dp)]

    def swap(arr):
        return lax.ppermute(arr, 'dp', pairs)

    def gather(arr):
        return lax.all_gather(arr, 'fsdp', axis=0, tiled=True)

    def local_fn(tokens, weights):
        w_query, w_key, w_value, w_out, w_gate, w_up, w_down, g_query, g_key, g_attn, g_mlp = weights
        part = lax.rem(lax.axis_index('dp'), 2)
        n_layers, rows, width = w_query.shape
        ff = w_gate.shape[2]
        down_rows = w_down.shape[1]
        n_seq, seq_len, _ = tokens.shape
        n_tok = n_seq * seq_len
        half = width // 2
        n_heads = half // HEAD_DIM
        cos_tab, sin_tab = rope_tables(seq_len)

        def my_half(arr, axis):
            size = arr.shape[axis] // 2
            return lax.dynamic_slice_in_dim(arr, part * size, size, axis)

        gains = jnp.concatenate([g_query, g_key, g_attn, g_mlp], axis=0)
        gains = lax.all_gather(gains, 'fsdp', axis=1, tiled=True).astype(jnp.float32)

        def gain(kind, layer):
            return gains[kind * n_layers + layer]

        full_w = []
        for layer in range(n_layers):
            qkv = jnp.concatenate([my_half(w[layer], 1) for w in (w_query, w_key, w_value)], axis=1)
            gate_up = jnp.concatenate([
                my_half(w[layer].reshape(rows, n_fsdp, ff // n_fsdp), 2).reshape(rows, ff // 2)
                for w in (w_gate, w_up)], axis=1)
            down = my_half(w_down[layer], 0)
            full_w.append([gather(qkv), gather(w_out[layer]), gather(gate_up),
                           [gather(down[:, :half]), gather(down[:, half:])] if layer == n_layers - 1 else [gather(down)]])

        own = tokens.reshape(n_tok, width)
        for layer in range(n_layers):
            qkv_w, out_w, gu_w, down_w = full_w[layer]
            both = jnp.concatenate([own, swap(own)], axis=0)
            lin = dot_bf16(both, qkv_w)
            q_lin = lin[:, :half].astype(jnp.float32)
            k_lin = lin[:, half:2 * half].astype(jnp.float32)
            v_heads = lin[:, 2 * half:].reshape(2 * n_seq, seq_len, n_heads, HEAD_DIM)
            stats = jnp.stack([jnp.sum(q_lin * q_lin, axis=-1), jnp.sum(k_lin * k_lin, axis=-1)])
            other = jnp.roll(swap(stats), n_tok, axis=1)
            inv = lax.rsqrt((stats + other) / width + EPS)

            def norm_rope(vals, inv_rms, gain_vec):
                normed = vals * inv_rms[:, None] * gain_vec
                normed = normed.reshape(2 * n_seq, seq_len, n_heads, HEAD_DIM)
                return apply_rope(normed, cos_tab, sin_tab).astype(jnp.bfloat16)

            q_rot = norm_rope(q_lin, inv[0], my_half(gain(0, layer), 0))
            k_rot = norm_rope(k_lin, inv[1], my_half(gain(1, layer), 0))
            attn = causal_attention(q_rot, k_rot, v_heads).reshape(2 * n_tok, half)
            mine, theirs = attn[:n_tok], swap(attn[n_tok:])
            attn_own = jnp.where(part == 0, jnp.concatenate([mine, theirs], axis=1), jnp.concatenate([theirs, mine], axis=1))
            hidden = residual_norm(own, dot_bf16(attn_own, out_w), gain(2, layer))
            hidden_other = swap(hidden)

            def mlp_mid(hid):
                gate_up = dot_bf16(hid, gu_w)
                gate = gate_up[:, :ff // 2].astype(jnp.float32)
                up = gate_up[:, ff // 2:].astype(jnp.float32)
                return (jax.nn.silu(gate) * up).astype(jnp.bfloat16)

            mid_own = mlp_mid(hidden)
            mid_other = mlp_mid(hidden_other)
            sums = []
            for piece in down_w:
                theirs_sum = swap(dot_f32(mid_other, piece))
                sums.append(dot_f32(mid_own, piece) + theirs_sum)
            down_lin = jnp.concatenate(sums, axis=1) if len(sums) > 1 else sums[0]
            own = residual_norm(hidden, down_lin, gain(3, layer))
        return own.reshape(n_seq, seq_len, width)

    mapped = jax.shard_map(local_fn, mesh=mesh, in_specs=(P(('dp', 'fsdp')), P(None, 'fsdp')), out_specs=P(('dp', 'fsdp')), check_vma=False)

    def run(tokens, w_query, w_key, w_value, w_out, w_gate, w_up, w_down, g_query, g_key, g_attn, g_mlp):
        return mapped(tokens, (w_query, w_key, w_value, w_out, w_gate, w_up, w_down, g_query, g_key, g_attn, g_mlp))

    return run
```

```python
import functools

import jax
import jax.numpy as jnp
import numpy as np
from jax import lax
from jax.experimental import pallas as pl
from jax.experimental.pallas import tpu as pltpu
from jax.sharding import PartitionSpec as P

HEAD_DIM = 128
EPS = 1e-6
THETA = 500000.0
SLAB = 1024
AHEAD = 2
LAG = 2
F32 = jnp.float32
BF16 = jnp.bfloat16


def rope_tables(seq_len):
    positions = np.arange(seq_len, dtype=np.float32)
    inv_freq = np.power(np.float32(THETA), -2.0 * np.arange(HEAD_DIM // 2, dtype=np.float32) / np.float32(HEAD_DIM)).astype(np.float32)
    angles = positions[:, None] * inv_freq[None, :]
    cos, sin = np.cos(angles), np.sin(angles)
    return np.concatenate([cos, cos], axis=1), np.concatenate([-sin, sin], axis=1)


def dot(left, right):
    return jnp.dot(left, right, preferred_element_type=F32)


def kernel(dims, tokens, gains, cos_ref, sin_ref, wq, wk, wv, wo, wg, wu, wd, out, gat,
           x2, qkv, att, att_in, alin, h2, mid, p_own, p_out, p_in, wbuf, stat, stat_in, gvec,
           sem_a, sem_b, sem_c, sem_s, sem_w, sem_g, sem_y, sem_p, sem_l):
    n, n_layers, n_tok, seq_len, width, rows, ff_blk, d_rows = dims
    half = width // 2
    n_heads = half // HEAD_DIM
    n_qkv, n_out, n_gu, n_down = 3, width // SLAB, n, width // 512
    per_layer = n_qkv + n_out + n_gu + n_down
    n_stage = per_layer * n_layers
    first_out, first_gu, first_down = n_qkv, n_qkv + n_out, n_qkv + n_out + n_gu
    me = lax.axis_index('fsdp')
    group = lax.axis_index('dp')
    part = lax.rem(group, 2)
    pair = {'dp': group + 1 - 2 * part}
    left = lax.rem(me + n - 2, n)
    right = lax.rem(me + 2, n)
    far = lax.rem(me + 4, n)
    sib = me + 1 - 2 * lax.rem(me, 2)
    own_rows = pl.ds(0, n_tok)
    pair_rows = pl.ds(n_tok, n_tok)

    def send(src, dst, s_sem, r_sem, dev):
        copy = pltpu.make_async_remote_copy(src_ref=src, dst_ref=dst, send_sem=s_sem, recv_sem=r_sem, device_id=dev,
                                            device_id_type=pl.DeviceIdType.MESH)
        copy.start()
        return copy

    def arrive(ref, sem):
        pltpu.make_async_copy(ref, ref, sem).wait()

    def own_blocks(layer, pos, do):
        for i, w in enumerate((wq, wk, wv)):
            @pl.when(pos == i)
            def _(w=w):
                do(w.at[layer, :, pl.ds(pl.multiple_of(part * half, 128), half)], slice(0, SLAB))

        @pl.when(jnp.logical_and(pos >= first_out, pos < first_gu))
        def _():
            do(wo.at[layer, :, pl.ds(pl.multiple_of((pos - first_out) * SLAB, 128), SLAB)], slice(0, SLAB))

        @pl.when(jnp.logical_and(pos >= first_gu, pos < first_down))
        def _():
            cols = pl.ds(pl.multiple_of((pos - first_gu) * 2 * ff_blk + part * ff_blk, 128), ff_blk)
            do(wg.at[layer, :, cols], slice(0, ff_blk))
            do(wu.at[layer, :, cols], slice(ff_blk, 2 * ff_blk))

        @pl.when(pos >= first_down)
        def _():
            cols = pl.ds(pl.multiple_of((pos - first_down) * 512, 128), 512)
            for k in range(2):
                do(wd.at[layer, pl.ds(pl.multiple_of(part * d_rows + k * rows, 128), rows), cols], slice(k * 512, (k + 1) * 512))

    def start_own(s):
        def do(src, cols):
            dst = gat.at[s, me, :, cols]
            send(src, dst, sem_s.at[s], sem_a.at[s], {'fsdp': right})
            send(src, dst, sem_s.at[s], sem_a.at[s], {'fsdp': left})
            send(src, dst, sem_s.at[s], sem_c.at[s], {'fsdp': sib})
        own_blocks(s // per_layer, lax.rem(s, per_layer), do)

    def pump(s):
        @pl.when(s < n_stage)
        def _():
            arrive(gat.at[s, pl.ds(0, 2)], sem_a.at[s])
            top, bottom = pl.ds(0, rows // 2), pl.ds(rows // 2, rows // 2)
            block = gat.at[s, left, top]
            send(block, block, sem_s.at[s], sem_b.at[s], {'fsdp': right})
            block = gat.at[s, right, bottom]
            send(block, block, sem_s.at[s], sem_b.at[s], {'fsdp': left})
            for origin in (left, right):
                block = gat.at[s, origin]
                send(block, block, sem_s.at[s], sem_c.at[s], {'fsdp': sib})

        @pl.when(s + AHEAD < n_stage)
        def _():
            start_own(s + AHEAD)

        @pl.when(jnp.logical_and(s >= LAG, s < n_stage + LAG))
        def _():
            t = s - LAG
            block = gat.at[t, far]
            arrive(block, sem_b.at[t])
            send(block, block, sem_s.at[t], sem_c.at[t], {'fsdp': sib})

    def stage_ready(s):
        arrive(gat.at[s, pl.ds(0, 4)], sem_c.at[s])

    def load(layer, pos, slot):
        s = layer * per_layer + pos
        for k in range(1, n):
            d = lax.rem(me + k, n)
            pltpu.make_async_copy(gat.at[s, d], wbuf.at[slot, d], sem_w.at[slot]).start()
        own_blocks(layer, pos, lambda src, cols: pltpu.make_async_copy(src, wbuf.at[slot, me, :, cols], sem_w.at[slot]).start())

    def loaded(slot):
        arrive(wbuf.at[slot], sem_w.at[slot])

    def tiles(layer, first, count, repeat, compute, pumps):
        stage, fresh = repeat

        def fetch(it):
            pos = first + stage(it)

            @pl.when(fresh(it))
            def _():
                stage_ready(layer * per_layer + pos)
            load(layer, pos, lax.rem(it, 2))

        pumps(jnp.int32(0))
        fetch(jnp.int32(0))

        def body(it, carry):
            @pl.when(it + 1 < count)
            def _():
                pumps(it + 1)
                fetch(it + 1)
            slot = lax.rem(it, 2)
            loaded(slot)
            compute(it, slot)
            return carry
        lax.fori_loop(0, count, body, 0)

    def weight(slot, cols):
        return wbuf[slot, :, :, cols].reshape(n * rows, cols.stop - cols.start)

    barrier = pltpu.get_barrier_semaphore()
    for k in range(1, n):
        pl.semaphore_signal(barrier, inc=1, device_id={'fsdp': lax.rem(me + k, n)}, device_id_type=pl.DeviceIdType.MESH)
    pl.semaphore_signal(barrier, inc=1, device_id=pair, device_id_type=pl.DeviceIdType.MESH)
    pl.semaphore_wait(barrier, n)

    for s in range(AHEAD):
        start_own(jnp.int32(s))
    x_copy = send(tokens, x2.at[pair_rows], sem_y.at[0], sem_y.at[1], pair)
    my_gain = gvec.at[:, pl.ds(pl.multiple_of(me * rows, 128), rows)]
    gain_copies = [send(gains, my_gain, sem_g.at[0], sem_g.at[1], {'fsdp': lax.rem(me + k, n)}) for k in range(1, n)]
    local = [pltpu.make_async_copy(tokens, x2.at[own_rows], sem_l.at[0]), pltpu.make_async_copy(gains, my_gain, sem_l.at[1])]
    for c in local:
        c.start()
    for c in local:
        c.wait()
    gain_ref = gvec.at[:, pl.ds(0, (n - 1) * rows)]
    arrive(gain_ref, sem_g.at[0])
    arrive(gain_ref, sem_g.at[1])
    x_copy.wait_send()
    for s in range(3):
        pump(jnp.int32(s))

    blk = 64

    def pick_gain(row, cols):
        table = gvec[:, cols]
        chosen = lax.broadcasted_iota(jnp.int32, table.shape, 0) == row
        return jnp.sum(jnp.where(chosen, table, 0.0), axis=0, keepdims=True)

    def residual_norm(res, lin, dst, gain_row):
        gain = pick_gain(gain_row, slice(None))

        def body(i, carry):
            r = pl.ds(pl.multiple_of(i * blk, blk), blk)
            v = lin(r)
            inv = lax.rsqrt(jnp.mean(v * v, axis=-1, keepdims=True) + EPS)
            dst[r, :] = (res[r, :].astype(F32) + v * inv * gain).astype(BF16)
            return carry
        lax.fori_loop(0, n_tok // blk, body, 0)

    def layer_body(layer, carry):
        base = layer * per_layer

        def qkv_compute(it, slot):
            @pl.when(it == n_qkv)
            def _():
                arrive(x2.at[pair_rows], sem_y.at[1])
            kind = lax.rem(it, n_qkv)
            r = pl.ds(pl.multiple_of((it // n_qkv) * n_tok, n_tok), n_tok)
            for k in range(SLAB // 512):
                val = dot(x2[r, :], weight(slot, slice(k * 512, (k + 1) * 512))).astype(BF16)
                qkv[r, pl.ds(pl.multiple_of(kind * half + k * 512, 128), 512)] = val
                sq = val.astype(F32)
                ssq = jnp.sum(sq * sq, axis=-1, keepdims=True)
                if k == 0:
                    total = ssq
                else:
                    total = total + ssq
            lane = lax.broadcasted_iota(jnp.int32, (n_tok, 128), 1)
            spread = jnp.broadcast_to(total, (n_tok, 128))

            @pl.when(kind == 0)
            def _():
                stat[r, :] = spread

            @pl.when(kind == 1)
            def _():
                stat[r, :] = jnp.where(lane < 64, stat[r, :], spread)

        def qkv_pumps(it):
            @pl.when(it < n_qkv)
            def _():
                pump(base + 3 + it)
        tiles(layer, 0, 2 * n_qkv, (lambda it: lax.rem(it, n_qkv), lambda it: it < n_qkv), qkv_compute, qkv_pumps)

        copies = [send(stat.at[own_rows], stat_in.at[pair_rows], sem_y.at[2], sem_y.at[3], pair),
                  send(stat.at[pair_rows], stat_in.at[own_rows], sem_y.at[4], sem_y.at[5], pair)]
        pump(base + 6)
        for c in copies:
            c.wait()

        n_seq = n_tok // seq_len

        def attend(it, carry):
            seq = lax.rem(it + n_seq, 2 * n_seq)
            r = pl.ds(pl.multiple_of(seq * seq_len, seq_len), seq_len)
            sums = (stat[r, :] + stat_in[r, :]) * (1.0 / width)
            inv = lax.rsqrt(sums + EPS)
            inv_q, inv_k = inv[:, 0:1], inv[:, 64:65]
            causal = lax.broadcasted_iota(jnp.int32, (seq_len, seq_len), 0) >= lax.broadcasted_iota(jnp.int32, (seq_len, seq_len), 1)

            def norm_rope(vals, inv_rms, gain):
                v = vals.astype(F32) * inv_rms * gain
                return (v * cos_ref[...] + pltpu.roll(v, HEAD_DIM // 2, 1) * sin_ref[...]).astype(BF16)

            def head(h, c2):
                col = pl.multiple_of(h * HEAD_DIM, HEAD_DIM)
                gcol = pl.ds(pl.multiple_of(part * half + col, HEAD_DIM), HEAD_DIM)
                q = norm_rope(qkv[r, pl.ds(col, HEAD_DIM)], inv_q, pick_gain(layer, gcol))
                k = norm_rope(qkv[r, pl.ds(pl.multiple_of(half + col, HEAD_DIM), HEAD_DIM)], inv_k, pick_gain(n_layers + layer, gcol))
                v = qkv[r, pl.ds(pl.multiple_of(2 * half + col, HEAD_DIM), HEAD_DIM)]
                sc = lax.dot_general(q, k, (((1,), (1,)), ((), ())), preferred_element_type=F32) * HEAD_DIM ** -0.5
                sc = jnp.where(causal, sc, -jnp.inf)
                e = jnp.exp(sc - jnp.max(sc, axis=-1, keepdims=True))
                p = (e / jnp.sum(e, axis=-1, keepdims=True)).astype(BF16)
                att[r, pl.ds(col, HEAD_DIM)] = dot(p, v).astype(BF16)
                return c2
            lax.fori_loop(0, n_heads, head, 0)

            @pl.when(it < 3)
            def _():
                pump(base + 7 + it)

            @pl.when(it == n_seq - 1)
            def _():
                send(att.at[pair_rows], att_in, sem_y.at[6], sem_y.at[7], pair)
            return carry
        lax.fori_loop(0, 2 * n_seq, attend, 0)
        arrive(att_in, sem_y.at[6])
        arrive(att_in, sem_y.at[7])

        def out_compute(it, slot):
            q = n // 2
            for k in range(SLAB // 512):
                cols = slice(k * 512, (k + 1) * 512)
                w_mine = wbuf[slot, pl.ds(part * q, q), :, cols].reshape(q * rows, 512)
                w_theirs = wbuf[slot, pl.ds((1 - part) * q, q), :, cols].reshape(q * rows, 512)
                val = dot(att[own_rows, :], w_mine) + dot(att_in[...], w_theirs)
                alin[:, pl.ds(pl.multiple_of(it * SLAB + k * 512, 128), 512)] = val.astype(BF16)

        def out_pumps(it):
            @pl.when(it == 0)
            def _():
                pump(base + 10)
        tiles(layer, first_out, n_out, (lambda it: it, lambda it: it >= 0), out_compute, out_pumps)
        residual_norm(x2, lambda r: alin[r, :].astype(F32), h2, 2 * n_layers + layer)
        h_copy = send(h2.at[own_rows], h2.at[pair_rows], sem_y.at[8], sem_y.at[9], pair)

        def gu_compute(it, slot):
            @pl.when(it == n_gu)
            def _():
                h_copy.wait()
            d = lax.rem(it, n_gu)
            r = pl.ds(pl.multiple_of((it // n_gu) * n_tok, n_tok), n_tok)
            for k in range(2):
                w = ff_blk // 2
                g = dot(h2[r, :], weight(slot, slice(k * w, (k + 1) * w))).astype(BF16).astype(F32)
                u = dot(h2[r, :], weight(slot, slice(ff_blk + k * w, ff_blk + (k + 1) * w))).astype(BF16).astype(F32)
                mid[r, pl.ds(pl.multiple_of(k * n * rows + d * w, 128), w)] = (jax.nn.silu(g) * u).astype(BF16)

        def gu_pumps(it):
            @pl.when(jnp.logical_and(it >= 3, it < n_gu))
            def _():
                pump(base + 8 + it)

            @pl.when(jnp.logical_or(it == 11, it == 14))
            def _():
                pump(base + 16 + (it - 11) // 3)
        tiles(layer, first_gu, 2 * n_gu, (lambda it: lax.rem(it, n_gu), lambda it: it < n_gu), gu_compute, gu_pumps)

        def down_compute(it, slot):
            c = it // 2
            cols = pl.ds(pl.multiple_of(c * 512, 512), 512)
            mine = lax.rem(it, 2)
            r = pl.ds(pl.multiple_of((1 - mine) * n_tok, n_tok), n_tok)
            k_half = n * rows
            val = dot(mid[r, 0:k_half], weight(slot, slice(0, 512))) + dot(mid[r, k_half:2 * k_half], weight(slot, slice(512, 1024)))

            @pl.when(mine == 1)
            def _():
                p_own[:, cols] = val

            @pl.when(mine == 0)
            def _():
                p_out[:, cols] = val
                send(p_out.at[:, cols], p_in.at[:, cols], sem_p.at[0, c], sem_p.at[1, c], pair)

        def down_pumps(it):
            @pl.when(jnp.logical_or(it == 4, it == 6))
            def _():
                pump(base + 18 + (it - 4) // 2)
        tiles(layer, first_down, 2 * n_down, (lambda it: it // 2, lambda it: lax.rem(it, 2) == 0), down_compute, down_pumps)
        for c in range(n_down):
            for k in range(2):
                arrive(p_in.at[:, pl.ds(c * 512, 512)], sem_p.at[k, c])
        residual_norm(h2, lambda r: (p_own[r, :] + p_in[r, :]).astype(BF16).astype(F32), x2, 3 * n_layers + layer)

        @pl.when(layer + 1 < n_layers)
        def _():
            send(x2.at[own_rows], x2.at[pair_rows], sem_y.at[0], sem_y.at[1], pair).wait_send()
        return carry
    lax.fori_loop(0, n_layers, layer_body, 0)

    done = pltpu.make_async_copy(x2.at[own_rows], out, sem_l.at[0])
    done.start()
    done.wait()

    def drain(s, carry):
        arrive(gat.at[s, pl.ds(0, 7)], sem_s.at[s])
        return carry
    lax.fori_loop(0, n_stage, drain, 0)


def solution(mesh):
    n_fsdp = mesh.shape['fsdp']

    def local_fn(tokens, weights):
        w_query, w_key, w_value, w_out, w_gate, w_up, w_down, g_query, g_key, g_attn, g_mlp = weights
        n_layers, rows, width = w_query.shape
        n_seq, seq_len, _ = tokens.shape
        n_tok = n_seq * seq_len
        ff = w_gate.shape[2]
        half = width // 2
        ff_blk = ff // n_fsdp // 2
        d_rows = w_down.shape[1] // 2
        dims = (n_fsdp, n_layers, n_tok, seq_len, width, rows, ff_blk, d_rows)
        n_stage = n_layers * (3 + width // SLAB + n_fsdp + width // 512)
        gains = jnp.concatenate([g_query, g_key, g_attn, g_mlp], axis=0).astype(F32)
        cos_tab, sin_tab = rope_tables(seq_len)
        hbm = pl.BlockSpec(memory_space=pl.ANY)
        vmem = pl.BlockSpec(memory_space=pltpu.VMEM)
        result, _ = pl.pallas_call(
            functools.partial(kernel, dims),
            out_shape=(jax.ShapeDtypeStruct((n_tok, width), BF16), jax.ShapeDtypeStruct((n_stage, n_fsdp, rows, SLAB), BF16)),
            in_specs=[hbm, vmem, vmem, vmem] + [hbm] * 7,
            out_specs=(hbm, hbm),
            scratch_shapes=[
                pltpu.VMEM((2 * n_tok, width), BF16),
                pltpu.VMEM((2 * n_tok, 3 * half), BF16),
                pltpu.VMEM((2 * n_tok, half), BF16),
                pltpu.VMEM((n_tok, half), BF16),
                pltpu.VMEM((n_tok, width), BF16),
                pltpu.VMEM((2 * n_tok, width), BF16),
                pltpu.VMEM((2 * n_tok, ff // 2), BF16),
                pltpu.VMEM((n_tok, width), F32),
                pltpu.VMEM((n_tok, width), F32),
                pltpu.VMEM((n_tok, width), F32),
                pltpu.VMEM((2, n_fsdp, rows, SLAB), BF16),
                pltpu.VMEM((2 * n_tok, 128), F32),
                pltpu.VMEM((2 * n_tok, 128), F32),
                pltpu.VMEM((4 * n_layers, width), F32),
                pltpu.SemaphoreType.DMA((n_stage,)),
                pltpu.SemaphoreType.DMA((n_stage,)),
                pltpu.SemaphoreType.DMA((n_stage,)),
                pltpu.SemaphoreType.DMA((n_stage,)),
                pltpu.SemaphoreType.DMA((2,)),
                pltpu.SemaphoreType.DMA((2,)),
                pltpu.SemaphoreType.DMA((10,)),
                pltpu.SemaphoreType.DMA((2, width // 512)),
                pltpu.SemaphoreType.DMA((2,)),
            ],
            compiler_params=pltpu.CompilerParams(collective_id=0, has_side_effects=True, vmem_limit_bytes=62 * 1024 * 1024),
        )(tokens.reshape(n_tok, width), gains, jnp.asarray(cos_tab), jnp.asarray(sin_tab), w_query, w_key, w_value, w_out, w_gate, w_up, w_down)
        return result.reshape(n_seq, seq_len, width)

    mapped = jax.shard_map(local_fn, mesh=mesh, in_specs=(P(('dp', 'fsdp')), P(None, 'fsdp')), out_specs=P(('dp', 'fsdp')), check_vma=False)

    def run(tokens, w_query, w_key, w_value, w_out, w_gate, w_up, w_down, g_query, g_key, g_attn, g_mlp):
        return mapped(tokens, (w_query, w_key, w_value, w_out, w_gate, w_up, w_down, g_query, g_key, g_attn, g_mlp))

    return run
```

```python
import functools

import jax
import jax.numpy as jnp
import numpy as np
from jax import lax
from jax.experimental import pallas as pl
from jax.experimental.pallas import tpu as pltpu
from jax.sharding import PartitionSpec as P

HEAD_DIM = 128
EPS = 1e-6
THETA = 500000.0
SLAB = 1024
AHEAD = 3
LAG = 2
F32 = jnp.float32
BF16 = jnp.bfloat16


def rope_tables(seq_len):
    positions = np.arange(seq_len, dtype=np.float32)
    inv_freq = np.power(np.float32(THETA), -2.0 * np.arange(HEAD_DIM // 2, dtype=np.float32) / np.float32(HEAD_DIM)).astype(np.float32)
    angles = positions[:, None] * inv_freq[None, :]
    cos, sin = np.cos(angles), np.sin(angles)
    return np.concatenate([cos, cos], axis=1), np.concatenate([-sin, sin], axis=1)


def dot(left, right):
    return jnp.dot(left, right, preferred_element_type=F32)


def kernel(dims, tokens, gains, cos_ref, sin_ref, wq, wk, wv, wo, wg, wu, wd, out, gat,
           x2, qkv, att, att_in, alin, h2, mid, p_own, p_out, p_in, wbuf, stat, stat_in, gvec,
           sem_a, sem_b, sem_c, sem_s, sem_w, sem_g, sem_y, sem_p, sem_l):
    n, n_layers, n_tok, seq_len, width, rows, ff_blk, d_rows = dims
    half = width // 2
    n_heads = half // HEAD_DIM
    n_qkv, n_out, n_gu, n_down = 3, width // SLAB, n, width // 512
    per_layer = n_qkv + n_out + n_gu + n_down
    n_stage = per_layer * n_layers
    first_out, first_gu, first_down = n_qkv, n_qkv + n_out, n_qkv + n_out + n_gu
    me = lax.axis_index('fsdp')
    group = lax.axis_index('dp')
    part = lax.rem(group, 2)
    pair = {'dp': group + 1 - 2 * part}
    left = lax.rem(me + n - 2, n)
    right = lax.rem(me + 2, n)
    far = lax.rem(me + 4, n)
    sib = me + 1 - 2 * lax.rem(me, 2)
    own_rows = pl.ds(0, n_tok)
    pair_rows = pl.ds(n_tok, n_tok)

    def send(src, dst, s_sem, r_sem, dev):
        copy = pltpu.make_async_remote_copy(src_ref=src, dst_ref=dst, send_sem=s_sem, recv_sem=r_sem, device_id=dev,
                                            device_id_type=pl.DeviceIdType.MESH)
        copy.start()
        return copy

    def arrive(ref, sem):
        pltpu.make_async_copy(ref, ref, sem).wait()

    def own_blocks(layer, pos, do):
        for i, w in enumerate((wq, wk, wv)):
            @pl.when(pos == i)
            def _(w=w):
                do(w.at[layer, :, pl.ds(pl.multiple_of(part * half, 128), half)], slice(0, SLAB))

        @pl.when(jnp.logical_and(pos >= first_out, pos < first_gu))
        def _():
            do(wo.at[layer, :, pl.ds(pl.multiple_of((pos - first_out) * SLAB, 128), SLAB)], slice(0, SLAB))

        @pl.when(jnp.logical_and(pos >= first_gu, pos < first_down))
        def _():
            cols = pl.ds(pl.multiple_of((pos - first_gu) * 2 * ff_blk + part * ff_blk, 128), ff_blk)
            do(wg.at[layer, :, cols], slice(0, ff_blk))
            do(wu.at[layer, :, cols], slice(ff_blk, 2 * ff_blk))

        @pl.when(pos >= first_down)
        def _():
            cols = pl.ds(pl.multiple_of((pos - first_down) * 512, 128), 512)
            for k in range(2):
                do(wd.at[layer, pl.ds(pl.multiple_of(part * d_rows + k * rows, 128), rows), cols], slice(k * 512, (k + 1) * 512))

    def start_own(s):
        def do(src, cols):
            dst = gat.at[s, me, :, cols]
            send(src, dst, sem_s.at[s], sem_a.at[s], {'fsdp': right})
            send(src, dst, sem_s.at[s], sem_a.at[s], {'fsdp': left})
            send(src, dst, sem_s.at[s], sem_c.at[s], {'fsdp': sib})
        own_blocks(s // per_layer, lax.rem(s, per_layer), do)

    def pump(s):
        @pl.when(s < n_stage)
        def _():
            arrive(gat.at[s, pl.ds(0, 2)], sem_a.at[s])
            top, bottom = pl.ds(0, rows // 2), pl.ds(rows // 2, rows // 2)
            block = gat.at[s, left, top]
            send(block, block, sem_s.at[s], sem_b.at[s], {'fsdp': right})
            block = gat.at[s, right, bottom]
            send(block, block, sem_s.at[s], sem_b.at[s], {'fsdp': left})
            for origin in (left, right):
                block = gat.at[s, origin]
                send(block, block, sem_s.at[s], sem_c.at[s], {'fsdp': sib})

        @pl.when(s + AHEAD < n_stage)
        def _():
            start_own(s + AHEAD)

        @pl.when(jnp.logical_and(s >= LAG, s < n_stage + LAG))
        def _():
            t = s - LAG
            block = gat.at[t, far]
            arrive(block, sem_b.at[t])
            send(block, block, sem_s.at[t], sem_c.at[t], {'fsdp': sib})

    def stage_ready(s):
        arrive(gat.at[s, pl.ds(0, 4)], sem_c.at[s])

    def load(layer, pos, slot):
        s = layer * per_layer + pos
        for k in range(1, n):
            d = lax.rem(me + k, n)
            pltpu.make_async_copy(gat.at[s, d], wbuf.at[slot, d], sem_w.at[slot]).start()
        own_blocks(layer, pos, lambda src, cols: pltpu.make_async_copy(src, wbuf.at[slot, me, :, cols], sem_w.at[slot]).start())

    def loaded(slot):
        arrive(wbuf.at[slot], sem_w.at[slot])

    def tiles(layer, first, count, repeat, compute, pumps):
        stage, fresh = repeat

        def fetch(it):
            pos = first + stage(it)

            @pl.when(fresh(it))
            def _():
                stage_ready(layer * per_layer + pos)
            load(layer, pos, lax.rem(it, 2))

        pumps(jnp.int32(0))
        fetch(jnp.int32(0))

        def body(it, carry):
            @pl.when(it + 1 < count)
            def _():
                pumps(it + 1)
                fetch(it + 1)
            slot = lax.rem(it, 2)
            loaded(slot)
            compute(it, slot)
            return carry
        lax.fori_loop(0, count, body, 0)

    def weight(slot, cols):
        return wbuf[slot, :, :, cols].reshape(n * rows, cols.stop - cols.start)

    barrier = pltpu.get_barrier_semaphore()
    for k in range(1, n):
        pl.semaphore_signal(barrier, inc=1, device_id={'fsdp': lax.rem(me + k, n)}, device_id_type=pl.DeviceIdType.MESH)
    pl.semaphore_signal(barrier, inc=1, device_id=pair, device_id_type=pl.DeviceIdType.MESH)
    pl.semaphore_wait(barrier, n)

    for s in range(AHEAD):
        start_own(jnp.int32(s))
    x_copy = send(tokens, x2.at[pair_rows], sem_y.at[0], sem_y.at[1], pair)
    my_gain = gvec.at[:, pl.ds(pl.multiple_of(me * rows, 128), rows)]
    gain_copies = [send(gains, my_gain, sem_g.at[0], sem_g.at[1], {'fsdp': lax.rem(me + k, n)}) for k in range(1, n)]
    local = [pltpu.make_async_copy(tokens, x2.at[own_rows], sem_l.at[0]), pltpu.make_async_copy(gains, my_gain, sem_l.at[1])]
    for c in local:
        c.start()
    for c in local:
        c.wait()
    gain_ref = gvec.at[:, pl.ds(0, (n - 1) * rows)]
    arrive(gain_ref, sem_g.at[0])
    arrive(gain_ref, sem_g.at[1])
    x_copy.wait_send()
    for s in range(3):
        pump(jnp.int32(s))

    blk = 64

    def pick_gain(row, cols):
        table = gvec[:, cols]
        chosen = lax.broadcasted_iota(jnp.int32, table.shape, 0) == row
        return jnp.sum(jnp.where(chosen, table, 0.0), axis=0, keepdims=True)

    def residual_norm(res, lin, dst, gain_row):
        gain = pick_gain(gain_row, slice(None))

        def body(i, carry):
            r = pl.ds(pl.multiple_of(i * blk, blk), blk)
            v = lin(r)
            inv = lax.rsqrt(jnp.mean(v * v, axis=-1, keepdims=True) + EPS)
            dst[r, :] = (res[r, :].astype(F32) + v * inv * gain).astype(BF16)
            return carry
        lax.fori_loop(0, n_tok // blk, body, 0)

    def layer_body(layer, carry):
        base = layer * per_layer

        def pump_span(lo, hi):
            lo, hi = (jnp.where(layer == 0, *v) if isinstance(v, tuple) else v for v in (lo, hi))

            def one(s, c):
                pump(base + s)
                return c
            lax.fori_loop(lo, hi, one, 0)

        def qkv_compute(it, slot):
            @pl.when(it == n_qkv)
            def _():
                pump_span(5, (5, 7))
                arrive(x2.at[pair_rows], sem_y.at[1])
            kind = lax.rem(it, n_qkv)
            r = pl.ds(pl.multiple_of((it // n_qkv) * n_tok, n_tok), n_tok)
            for k in range(SLAB // 512):
                val = dot(x2[r, :], weight(slot, slice(k * 512, (k + 1) * 512))).astype(BF16)
                qkv[r, pl.ds(pl.multiple_of(kind * half + k * 512, 128), 512)] = val
                sq = val.astype(F32)
                ssq = jnp.sum(sq * sq, axis=-1, keepdims=True)
                if k == 0:
                    total = ssq
                else:
                    total = total + ssq
            lane = lax.broadcasted_iota(jnp.int32, (n_tok, 128), 1)
            spread = jnp.broadcast_to(total, (n_tok, 128))

            @pl.when(kind == 0)
            def _():
                stat[r, :] = spread

            @pl.when(kind == 1)
            def _():
                stat[r, :] = jnp.where(lane < 64, stat[r, :], spread)

        def qkv_pumps(it):
            @pl.when(it == 1)
            def _():
                pump_span((3, 4), 4)

            @pl.when(it == 2)
            def _():
                pump_span(4, 5)
        tiles(layer, 0, 2 * n_qkv, (lambda it: lax.rem(it, n_qkv), lambda it: it < n_qkv), qkv_compute, qkv_pumps)

        copies = [send(stat.at[own_rows], stat_in.at[pair_rows], sem_y.at[2], sem_y.at[3], pair),
                  send(stat.at[pair_rows], stat_in.at[own_rows], sem_y.at[4], sem_y.at[5], pair)]
        pump_span((5, 7), (6, 8))
        for c in copies:
            c.wait()

        n_seq = n_tok // seq_len

        def attend(it, carry):
            seq = lax.rem(it + n_seq, 2 * n_seq)
            r = pl.ds(pl.multiple_of(seq * seq_len, seq_len), seq_len)
            sums = (stat[r, :] + stat_in[r, :]) * (1.0 / width)
            inv = lax.rsqrt(sums + EPS)
            inv_q, inv_k = inv[:, 0:1], inv[:, 64:65]
            causal = lax.broadcasted_iota(jnp.int32, (seq_len, seq_len), 0) >= lax.broadcasted_iota(jnp.int32, (seq_len, seq_len), 1)

            def norm_rope(vals, inv_rms, gain):
                v = vals.astype(F32) * inv_rms * gain
                return (v * cos_ref[...] + pltpu.roll(v, HEAD_DIM // 2, 1) * sin_ref[...]).astype(BF16)

            def head(h, c2):
                col = pl.multiple_of(h * HEAD_DIM, HEAD_DIM)
                gcol = pl.ds(pl.multiple_of(part * half + col, HEAD_DIM), HEAD_DIM)
                q = norm_rope(qkv[r, pl.ds(col, HEAD_DIM)], inv_q, pick_gain(layer, gcol))
                k = norm_rope(qkv[r, pl.ds(pl.multiple_of(half + col, HEAD_DIM), HEAD_DIM)], inv_k, pick_gain(n_layers + layer, gcol))
                v = qkv[r, pl.ds(pl.multiple_of(2 * half + col, HEAD_DIM), HEAD_DIM)]
                sc = lax.dot_general(q, k, (((1,), (1,)), ((), ())), preferred_element_type=F32) * HEAD_DIM ** -0.5
                sc = jnp.where(causal, sc, -jnp.inf)
                e = jnp.exp(sc - jnp.max(sc, axis=-1, keepdims=True))
                p = (e / jnp.sum(e, axis=-1, keepdims=True)).astype(BF16)
                att[r, pl.ds(col, HEAD_DIM)] = dot(p, v).astype(BF16)
                return c2
            lax.fori_loop(0, n_heads, head, 0)

            @pl.when(it == n_seq - 1)
            def _():
                send(att.at[pair_rows], att_in, sem_y.at[6], sem_y.at[7], pair)

            @pl.when(it == 1)
            def _():
                pump_span((6, 8), (7, 9))

            @pl.when(it == 3)
            def _():
                pump_span((7, 9), (7, 10))
            return carry
        lax.fori_loop(0, 2 * n_seq, attend, 0)
        arrive(att_in, sem_y.at[6])
        arrive(att_in, sem_y.at[7])

        def out_compute(it, slot):
            q = n // 2
            for k in range(SLAB // 512):
                cols = slice(k * 512, (k + 1) * 512)
                w_mine = wbuf[slot, pl.ds(part * q, q), :, cols].reshape(q * rows, 512)
                w_theirs = wbuf[slot, pl.ds((1 - part) * q, q), :, cols].reshape(q * rows, 512)
                val = dot(att[own_rows, :], w_mine) + dot(att_in[...], w_theirs)
                alin[:, pl.ds(pl.multiple_of(it * SLAB + k * 512, 128), 512)] = val.astype(BF16)

        def out_pumps(it):
            return
        tiles(layer, first_out, n_out, (lambda it: it, lambda it: it >= 0), out_compute, out_pumps)
        residual_norm(x2, lambda r: alin[r, :].astype(F32), h2, 2 * n_layers + layer)
        h_copy = send(h2.at[own_rows], h2.at[pair_rows], sem_y.at[8], sem_y.at[9], pair)
        pump_span((7, 10), (7, 11))

        def gu_compute(it, slot):
            @pl.when(it == n_gu)
            def _():
                h_copy.wait()
            d = lax.rem(it, n_gu)
            r = pl.ds(pl.multiple_of((it // n_gu) * n_tok, n_tok), n_tok)
            for k in range(2):
                w = ff_blk // 2
                g = dot(h2[r, :], weight(slot, slice(k * w, (k + 1) * w))).astype(BF16).astype(F32)
                u = dot(h2[r, :], weight(slot, slice(ff_blk + k * w, ff_blk + (k + 1) * w))).astype(BF16).astype(F32)
                mid[r, pl.ds(pl.multiple_of(k * n * rows + d * w, 128), w)] = (jax.nn.silu(g) * u).astype(BF16)

        def gu_pumps(it):
            @pl.when(it < n_gu)
            def _():
                pump_span((7 + it, jnp.where(it < 4, 11, 7 + it)), (8 + it, jnp.where(it < 4, 11, 8 + it)))
        tiles(layer, first_gu, 2 * n_gu, (lambda it: lax.rem(it, n_gu), lambda it: it < n_gu), gu_compute, gu_pumps)

        def down_compute(it, slot):
            c = it // 2
            cols = pl.ds(pl.multiple_of(c * 512, 512), 512)
            mine = lax.rem(it, 2)
            r = pl.ds(pl.multiple_of((1 - mine) * n_tok, n_tok), n_tok)
            k_half = n * rows
            val = dot(mid[r, 0:k_half], weight(slot, slice(0, 512))) + dot(mid[r, k_half:2 * k_half], weight(slot, slice(512, 1024)))

            @pl.when(mine == 1)
            def _():
                p_own[:, cols] = val

            @pl.when(mine == 0)
            def _():
                p_out[:, cols] = val
                send(p_out.at[:, cols], p_in.at[:, cols], sem_p.at[0, c], sem_p.at[1, c], pair)

        def down_pumps(it):
            @pl.when(lax.rem(it, 2) == 0)
            def _():
                pump_span(15 + it // 2, 16 + it // 2)
        tiles(layer, first_down, 2 * n_down, (lambda it: it // 2, lambda it: lax.rem(it, 2) == 0), down_compute, down_pumps)
        pump_span(19, 21)
        for c in range(n_down):
            for k in range(2):
                arrive(p_in.at[:, pl.ds(c * 512, 512)], sem_p.at[k, c])
        residual_norm(h2, lambda r: (p_own[r, :] + p_in[r, :]).astype(BF16).astype(F32), x2, 3 * n_layers + layer)

        @pl.when(layer + 1 < n_layers)
        def _():
            send(x2.at[own_rows], x2.at[pair_rows], sem_y.at[0], sem_y.at[1], pair).wait_send()
        return carry
    lax.fori_loop(0, n_layers, layer_body, 0)

    done = pltpu.make_async_copy(x2.at[own_rows], out, sem_l.at[0])
    done.start()
    done.wait()

    def drain(s, carry):
        arrive(gat.at[s, pl.ds(0, 7)], sem_s.at[s])
        return carry
    lax.fori_loop(0, n_stage, drain, 0)


def solution(mesh):
    n_fsdp = mesh.shape['fsdp']

    def local_fn(tokens, weights):
        w_query, w_key, w_value, w_out, w_gate, w_up, w_down, g_query, g_key, g_attn, g_mlp = weights
        n_layers, rows, width = w_query.shape
        n_seq, seq_len, _ = tokens.shape
        n_tok = n_seq * seq_len
        ff = w_gate.shape[2]
        half = width // 2
        ff_blk = ff // n_fsdp // 2
        d_rows = w_down.shape[1] // 2
        dims = (n_fsdp, n_layers, n_tok, seq_len, width, rows, ff_blk, d_rows)
        n_stage = n_layers * (3 + width // SLAB + n_fsdp + width // 512)
        gains = jnp.concatenate([g_query, g_key, g_attn, g_mlp], axis=0).astype(F32)
        cos_tab, sin_tab = rope_tables(seq_len)
        hbm = pl.BlockSpec(memory_space=pl.ANY)
        vmem = pl.BlockSpec(memory_space=pltpu.VMEM)
        result, _ = pl.pallas_call(
            functools.partial(kernel, dims),
            out_shape=(jax.ShapeDtypeStruct((n_tok, width), BF16), jax.ShapeDtypeStruct((n_stage, n_fsdp, rows, SLAB), BF16)),
            in_specs=[hbm, vmem, vmem, vmem] + [hbm] * 7,
            out_specs=(hbm, hbm),
            scratch_shapes=[
                pltpu.VMEM((2 * n_tok, width), BF16),
                pltpu.VMEM((2 * n_tok, 3 * half), BF16),
                pltpu.VMEM((2 * n_tok, half), BF16),
                pltpu.VMEM((n_tok, half), BF16),
                pltpu.VMEM((n_tok, width), BF16),
                pltpu.VMEM((2 * n_tok, width), BF16),
                pltpu.VMEM((2 * n_tok, ff // 2), BF16),
                pltpu.VMEM((n_tok, width), F32),
                pltpu.VMEM((n_tok, width), F32),
                pltpu.VMEM((n_tok, width), F32),
                pltpu.VMEM((2, n_fsdp, rows, SLAB), BF16),
                pltpu.VMEM((2 * n_tok, 128), F32),
                pltpu.VMEM((2 * n_tok, 128), F32),
                pltpu.VMEM((4 * n_layers, width), F32),
                pltpu.SemaphoreType.DMA((n_stage,)),
                pltpu.SemaphoreType.DMA((n_stage,)),
                pltpu.SemaphoreType.DMA((n_stage,)),
                pltpu.SemaphoreType.DMA((n_stage,)),
                pltpu.SemaphoreType.DMA((2,)),
                pltpu.SemaphoreType.DMA((2,)),
                pltpu.SemaphoreType.DMA((10,)),
                pltpu.SemaphoreType.DMA((2, width // 512)),
                pltpu.SemaphoreType.DMA((2,)),
            ],
            compiler_params=pltpu.CompilerParams(collective_id=0, has_side_effects=True, vmem_limit_bytes=62 * 1024 * 1024),
        )(tokens.reshape(n_tok, width), gains, jnp.asarray(cos_tab), jnp.asarray(sin_tab), w_query, w_key, w_value, w_out, w_gate, w_up, w_down)
        return result.reshape(n_seq, seq_len, width)

    mapped = jax.shard_map(local_fn, mesh=mesh, in_specs=(P(('dp', 'fsdp')), P(None, 'fsdp')), out_specs=P(('dp', 'fsdp')), check_vma=False)

    def run(tokens, w_query, w_key, w_value, w_out, w_gate, w_up, w_down, g_query, g_key, g_attn, g_mlp):
        return mapped(tokens, (w_query, w_key, w_value, w_out, w_gate, w_up, w_down, g_query, g_key, g_attn, g_mlp))

    return run
```

```python
import functools

import jax
import jax.numpy as jnp
import numpy as np
from jax import lax
from jax.experimental import pallas as pl
from jax.experimental.pallas import tpu as pltpu
from jax.sharding import PartitionSpec as P

HEAD_DIM = 128
EPS = 1e-6
THETA = 500000.0
SLAB = 1024
AHEAD = 3
LAG = 2
F32 = jnp.float32
BF16 = jnp.bfloat16


def rope_tables(seq_len):
    positions = np.arange(seq_len, dtype=np.float32)
    inv_freq = np.power(np.float32(THETA), -2.0 * np.arange(HEAD_DIM // 2, dtype=np.float32) / np.float32(HEAD_DIM)).astype(np.float32)
    angles = positions[:, None] * inv_freq[None, :]
    cos, sin = np.cos(angles), np.sin(angles)
    return np.concatenate([cos, cos], axis=1), np.concatenate([-sin, sin], axis=1)


def dot(left, right):
    return jnp.dot(left, right, preferred_element_type=F32)


def kernel(dims, tokens, gains, cos_ref, sin_ref, wq, wk, wv, wo, wg, wu, wd, out, gat,
           x2, qkv, att, att_in, alin, h2, mid, p_own, p_out, p_in, wbuf, stat, stat_in, gvec,
           sem_a, sem_b, sem_c, sem_s, sem_w, sem_g, sem_y, sem_p, sem_l):
    n, n_layers, n_tok, seq_len, width, rows, ff_blk, d_rows = dims
    half = width // 2
    n_heads = half // HEAD_DIM
    n_qkv, n_out, n_gu, n_down = 3, width // SLAB, n, width // 512
    per_layer = n_qkv + n_out + n_gu + n_down
    n_stage = per_layer * n_layers
    first_out, first_gu, first_down = n_qkv, n_qkv + n_out, n_qkv + n_out + n_gu
    me = lax.axis_index('fsdp')
    group = lax.axis_index('dp')
    part = lax.rem(group, 2)
    pair = {'dp': group + 1 - 2 * part}
    left = lax.rem(me + n - 2, n)
    right = lax.rem(me + 2, n)
    far = lax.rem(me + 4, n)
    sib = me + 1 - 2 * lax.rem(me, 2)
    own_rows = pl.ds(0, n_tok)
    pair_rows = pl.ds(n_tok, n_tok)

    def send(src, dst, s_sem, r_sem, dev):
        copy = pltpu.make_async_remote_copy(src_ref=src, dst_ref=dst, send_sem=s_sem, recv_sem=r_sem, device_id=dev,
                                            device_id_type=pl.DeviceIdType.MESH)
        copy.start()
        return copy

    def arrive(ref, sem):
        pltpu.make_async_copy(ref, ref, sem).wait()

    def own_blocks(layer, pos, do):
        for i, w in enumerate((wq, wk, wv)):
            @pl.when(pos == i)
            def _(w=w):
                do(w.at[layer, :, pl.ds(pl.multiple_of(part * half, 128), half)], slice(0, SLAB))

        @pl.when(jnp.logical_and(pos >= first_out, pos < first_gu))
        def _():
            do(wo.at[layer, :, pl.ds(pl.multiple_of((pos - first_out) * SLAB, 128), SLAB)], slice(0, SLAB))

        @pl.when(jnp.logical_and(pos >= first_gu, pos < first_down))
        def _():
            cols = pl.ds(pl.multiple_of((pos - first_gu) * 2 * ff_blk + part * ff_blk, 128), ff_blk)
            do(wg.at[layer, :, cols], slice(0, ff_blk))
            do(wu.at[layer, :, cols], slice(ff_blk, 2 * ff_blk))

        @pl.when(pos >= first_down)
        def _():
            cols = pl.ds(pl.multiple_of((pos - first_down) * 512, 128), 512)
            for k in range(2):
                do(wd.at[layer, pl.ds(pl.multiple_of(part * d_rows + k * rows, 128), rows), cols], slice(k * 512, (k + 1) * 512))

    def start_own(s):
        def do(src, cols):
            dst = gat.at[s, me, :, cols]
            send(src, dst, sem_s.at[s], sem_a.at[s], {'fsdp': right})
            send(src, dst, sem_s.at[s], sem_a.at[s], {'fsdp': left})
            send(src, dst, sem_s.at[s], sem_c.at[s], {'fsdp': sib})
        own_blocks(s // per_layer, lax.rem(s, per_layer), do)

    def pump(s):
        @pl.when(s < n_stage)
        def _():
            arrive(gat.at[s, pl.ds(0, 2)], sem_a.at[s])
            top, bottom = pl.ds(0, rows // 2), pl.ds(rows // 2, rows // 2)
            block = gat.at[s, left, top]
            send(block, block, sem_s.at[s], sem_b.at[s], {'fsdp': right})
            block = gat.at[s, right, bottom]
            send(block, block, sem_s.at[s], sem_b.at[s], {'fsdp': left})
            for origin in (left, right):
                block = gat.at[s, origin]
                send(block, block, sem_s.at[s], sem_c.at[s], {'fsdp': sib})

        @pl.when(s + AHEAD < n_stage)
        def _():
            start_own(s + AHEAD)

        @pl.when(jnp.logical_and(s >= LAG, s < n_stage + LAG))
        def _():
            t = s - LAG
            block = gat.at[t, far]
            arrive(block, sem_b.at[t])
            send(block, block, sem_s.at[t], sem_c.at[t], {'fsdp': sib})

    def stage_ready(s):
        arrive(gat.at[s, pl.ds(0, 4)], sem_c.at[s])

    def load(layer, pos, slot):
        s = layer * per_layer + pos
        for k in range(1, n):
            d = lax.rem(me + k, n)
            pltpu.make_async_copy(gat.at[s, d], wbuf.at[slot, d], sem_w.at[slot]).start()
        own_blocks(layer, pos, lambda src, cols: pltpu.make_async_copy(src, wbuf.at[slot, me, :, cols], sem_w.at[slot]).start())

    def loaded(slot):
        arrive(wbuf.at[slot], sem_w.at[slot])

    def tiles(layer, first, count, repeat, compute, pumps):
        stage, fresh = repeat

        def fetch(it):
            pos = first + stage(it)

            @pl.when(fresh(it))
            def _():
                stage_ready(layer * per_layer + pos)
            load(layer, pos, lax.rem(it, 2))

        pumps(jnp.int32(0))
        fetch(jnp.int32(0))

        def body(it, carry):
            @pl.when(it + 1 < count)
            def _():
                pumps(it + 1)
                fetch(it + 1)
            slot = lax.rem(it, 2)
            loaded(slot)
            compute(it, slot)
            return carry
        lax.fori_loop(0, count, body, 0)

    def weight(slot, cols):
        return wbuf[slot, :, :, cols].reshape(n * rows, cols.stop - cols.start)

    barrier = pltpu.get_barrier_semaphore()
    for k in range(1, n):
        pl.semaphore_signal(barrier, inc=1, device_id={'fsdp': lax.rem(me + k, n)}, device_id_type=pl.DeviceIdType.MESH)
    pl.semaphore_signal(barrier, inc=1, device_id=pair, device_id_type=pl.DeviceIdType.MESH)
    pl.semaphore_wait(barrier, n)

    for s in range(AHEAD):
        start_own(jnp.int32(s))
    my_gain = gvec.at[:, pl.ds(pl.multiple_of(me * rows, 128), rows)]
    gain_copies = [send(gains, my_gain, sem_g.at[0], sem_g.at[1], {'fsdp': lax.rem(me + k, n)}) for k in range(1, n)]
    local = [pltpu.make_async_copy(tokens, x2.at[own_rows], sem_l.at[0]), pltpu.make_async_copy(gains, my_gain, sem_l.at[1])]
    for c in local:
        c.start()
    for c in local:
        c.wait()
    gain_ref = gvec.at[:, pl.ds(0, (n - 1) * rows)]
    arrive(gain_ref, sem_g.at[0])
    arrive(gain_ref, sem_g.at[1])
    for s in range(3):
        pump(jnp.int32(s))

    blk = 64

    def pick_gain(row, cols):
        table = gvec[:, cols]
        chosen = lax.broadcasted_iota(jnp.int32, table.shape, 0) == row
        return jnp.sum(jnp.where(chosen, table, 0.0), axis=0, keepdims=True)

    def residual_norm(res, lin, dst, gain_row):
        gain = pick_gain(gain_row, slice(None))

        def body(i, carry):
            r = pl.ds(pl.multiple_of(i * blk, blk), blk)
            v = lin(r)
            inv = lax.rsqrt(jnp.mean(v * v, axis=-1, keepdims=True) + EPS)
            dst[r, :] = (res[r, :].astype(F32) + v * inv * gain).astype(BF16)
            return carry
        lax.fori_loop(0, n_tok // blk, body, 0)

    def layer_body(layer, carry):
        base = layer * per_layer

        def pump_span(lo, hi):
            lo, hi = (jnp.where(layer == 0, *v) if isinstance(v, tuple) else v for v in (lo, hi))

            def one(s, c):
                pump(base + s)
                return c
            lax.fori_loop(lo, hi, one, 0)

        x_copy = send(x2.at[own_rows], x2.at[pair_rows], sem_y.at[0], sem_y.at[1], pair)

        def qkv_compute(it, slot):
            @pl.when(it == n_qkv)
            def _():
                pump_span(5, (5, 7))
                x_copy.wait_recv()
            kind = lax.rem(it, n_qkv)
            r = pl.ds(pl.multiple_of((it // n_qkv) * n_tok, n_tok), n_tok)
            for k in range(SLAB // 512):
                val = dot(x2[r, :], weight(slot, slice(k * 512, (k + 1) * 512))).astype(BF16)
                qkv[r, pl.ds(pl.multiple_of(kind * half + k * 512, 128), 512)] = val
                sq = val.astype(F32)
                ssq = jnp.sum(sq * sq, axis=-1, keepdims=True)
                if k == 0:
                    total = ssq
                else:
                    total = total + ssq
            lane = lax.broadcasted_iota(jnp.int32, (n_tok, 128), 1)
            spread = jnp.broadcast_to(total, (n_tok, 128))

            @pl.when(kind == 0)
            def _():
                stat[r, :] = spread

            @pl.when(kind == 1)
            def _():
                stat[r, :] = jnp.where(lane < 64, stat[r, :], spread)

        def qkv_pumps(it):
            @pl.when(it == 1)
            def _():
                pump_span((3, 4), 4)

            @pl.when(it == 2)
            def _():
                pump_span(4, 5)
        tiles(layer, 0, 2 * n_qkv, (lambda it: lax.rem(it, n_qkv), lambda it: it < n_qkv), qkv_compute, qkv_pumps)

        copies = [send(stat.at[own_rows], stat_in.at[pair_rows], sem_y.at[2], sem_y.at[3], pair),
                  send(stat.at[pair_rows], stat_in.at[own_rows], sem_y.at[4], sem_y.at[5], pair)]
        pump_span((5, 7), (6, 8))
        for c in copies:
            c.wait()

        n_seq = n_tok // seq_len

        def attend(it, carry):
            seq = lax.rem(it + n_seq, 2 * n_seq)
            r = pl.ds(pl.multiple_of(seq * seq_len, seq_len), seq_len)
            sums = (stat[r, :] + stat_in[r, :]) * (1.0 / width)
            inv = lax.rsqrt(sums + EPS)
            inv_q, inv_k = inv[:, 0:1], inv[:, 64:65]
            causal = lax.broadcasted_iota(jnp.int32, (seq_len, seq_len), 0) >= lax.broadcasted_iota(jnp.int32, (seq_len, seq_len), 1)

            def norm_rope(vals, inv_rms, gain):
                v = vals.astype(F32) * inv_rms * gain
                return (v * cos_ref[...] + pltpu.roll(v, HEAD_DIM // 2, 1) * sin_ref[...]).astype(BF16)

            def head(h, c2):
                col = pl.multiple_of(h * HEAD_DIM, HEAD_DIM)
                gcol = pl.ds(pl.multiple_of(part * half + col, HEAD_DIM), HEAD_DIM)
                q = norm_rope(qkv[r, pl.ds(col, HEAD_DIM)], inv_q, pick_gain(layer, gcol))
                k = norm_rope(qkv[r, pl.ds(pl.multiple_of(half + col, HEAD_DIM), HEAD_DIM)], inv_k, pick_gain(n_layers + layer, gcol))
                v = qkv[r, pl.ds(pl.multiple_of(2 * half + col, HEAD_DIM), HEAD_DIM)]
                sc = lax.dot_general(q, k, (((1,), (1,)), ((), ())), preferred_element_type=F32) * HEAD_DIM ** -0.5
                sc = jnp.where(causal, sc, -jnp.inf)
                e = jnp.exp(sc - jnp.max(sc, axis=-1, keepdims=True))
                p = (e / jnp.sum(e, axis=-1, keepdims=True)).astype(BF16)
                att[r, pl.ds(col, HEAD_DIM)] = dot(p, v).astype(BF16)
                return c2
            lax.fori_loop(0, n_heads, head, 0)

            @pl.when(it == n_seq - 1)
            def _():
                send(att.at[pair_rows], att_in, sem_y.at[6], sem_y.at[7], pair)

            @pl.when(it == 1)
            def _():
                pump_span((6, 8), (7, 9))

            @pl.when(it == 3)
            def _():
                pump_span((7, 9), (7, 10))
            return carry
        lax.fori_loop(0, 2 * n_seq, attend, 0)
        arrive(att_in, sem_y.at[6])
        arrive(att_in, sem_y.at[7])

        def out_compute(it, slot):
            q = n // 2
            for k in range(SLAB // 512):
                cols = slice(k * 512, (k + 1) * 512)
                w_mine = wbuf[slot, pl.ds(part * q, q), :, cols].reshape(q * rows, 512)
                w_theirs = wbuf[slot, pl.ds((1 - part) * q, q), :, cols].reshape(q * rows, 512)
                val = dot(att[own_rows, :], w_mine) + dot(att_in[...], w_theirs)
                alin[:, pl.ds(pl.multiple_of(it * SLAB + k * 512, 128), 512)] = val.astype(BF16)

        def out_pumps(it):
            return
        tiles(layer, first_out, n_out, (lambda it: it, lambda it: it >= 0), out_compute, out_pumps)
        residual_norm(x2, lambda r: alin[r, :].astype(F32), h2, 2 * n_layers + layer)
        h_copy = send(h2.at[own_rows], h2.at[pair_rows], sem_y.at[8], sem_y.at[9], pair)
        pump_span((7, 10), (7, 11))

        n_early = n_gu - 2

        def gu_compute(d, theirs, slot):
            r = pl.ds(pl.multiple_of(theirs * n_tok, n_tok), n_tok)
            for k in range(2):
                w = ff_blk // 2
                g = dot(h2[r, :], weight(slot, slice(k * w, (k + 1) * w))).astype(BF16).astype(F32)
                u = dot(h2[r, :], weight(slot, slice(ff_blk + k * w, ff_blk + (k + 1) * w))).astype(BF16).astype(F32)
                mid[r, pl.ds(pl.multiple_of(k * n * rows + d * w, 128), w)] = (jax.nn.silu(g) * u).astype(BF16)

        def gu_early(it, slot):
            @pl.when(it == n_early)
            def _():
                h_copy.wait()
            gu_compute(lax.rem(it, n_early), it // n_early, slot)

        def early_pumps(it):
            @pl.when(it < n_early)
            def _():
                pump_span((7 + it, jnp.where(it < 4, 11, 7 + it)), (8 + it, jnp.where(it < 4, 11, 8 + it)))

            @pl.when(it == n_early)
            def _():
                pump_span(13, (13, 14))
        tiles(layer, first_gu, 2 * n_early, (lambda it: lax.rem(it, n_early), lambda it: it < n_early), gu_early, early_pumps)

        def late_pumps(it):
            @pl.when(it == 0)
            def _():
                pump_span((13, 14), 14)

            @pl.when(it == 2)
            def _():
                pump_span(14, 15)
        tiles(layer, first_gu + n_early, 2 * (n_gu - n_early), (lambda it: it // 2, lambda it: lax.rem(it, 2) == 0),
              lambda it, slot: gu_compute(n_early + it // 2, lax.rem(it, 2), slot), late_pumps)

        def down_compute(it, slot):
            c = it // 2
            cols = pl.ds(pl.multiple_of(c * 512, 512), 512)
            mine = lax.rem(it, 2)
            r = pl.ds(pl.multiple_of((1 - mine) * n_tok, n_tok), n_tok)
            k_half = n * rows
            val = dot(mid[r, 0:k_half], weight(slot, slice(0, 512))) + dot(mid[r, k_half:2 * k_half], weight(slot, slice(512, 1024)))

            @pl.when(mine == 1)
            def _():
                p_own[:, cols] = val

            @pl.when(mine == 0)
            def _():
                p_out[:, cols] = val
                send(p_out.at[:, cols], p_in.at[:, cols], sem_p.at[0, c], sem_p.at[1, c], pair)

        def down_pumps(it):
            @pl.when(lax.rem(it, 2) == 0)
            def _():
                pump_span(15 + it // 2, 16 + it // 2)
        tiles(layer, first_down, 2 * n_down, (lambda it: it // 2, lambda it: lax.rem(it, 2) == 0), down_compute, down_pumps)
        pump_span(19, 21)
        for c in range(n_down):
            for k in range(2):
                arrive(p_in.at[:, pl.ds(c * 512, 512)], sem_p.at[k, c])
        x_copy.wait_send()
        residual_norm(h2, lambda r: (p_own[r, :] + p_in[r, :]).astype(BF16).astype(F32), x2, 3 * n_layers + layer)
        return carry
    lax.fori_loop(0, n_layers, layer_body, 0)

    done = pltpu.make_async_copy(x2.at[own_rows], out, sem_l.at[0])
    done.start()
    done.wait()

    def drain(s, carry):
        arrive(gat.at[s, pl.ds(0, 7)], sem_s.at[s])
        return carry
    lax.fori_loop(0, n_stage, drain, 0)


def solution(mesh):
    n_fsdp = mesh.shape['fsdp']

    def local_fn(tokens, weights):
        w_query, w_key, w_value, w_out, w_gate, w_up, w_down, g_query, g_key, g_attn, g_mlp = weights
        n_layers, rows, width = w_query.shape
        n_seq, seq_len, _ = tokens.shape
        n_tok = n_seq * seq_len
        ff = w_gate.shape[2]
        half = width // 2
        ff_blk = ff // n_fsdp // 2
        d_rows = w_down.shape[1] // 2
        dims = (n_fsdp, n_layers, n_tok, seq_len, width, rows, ff_blk, d_rows)
        n_stage = n_layers * (3 + width // SLAB + n_fsdp + width // 512)
        gains = jnp.concatenate([g_query, g_key, g_attn, g_mlp], axis=0).astype(F32)
        cos_tab, sin_tab = rope_tables(seq_len)
        hbm = pl.BlockSpec(memory_space=pl.ANY)
        vmem = pl.BlockSpec(memory_space=pltpu.VMEM)
        result, _ = pl.pallas_call(
            functools.partial(kernel, dims),
            out_shape=(jax.ShapeDtypeStruct((n_tok, width), BF16), jax.ShapeDtypeStruct((n_stage, n_fsdp, rows, SLAB), BF16)),
            in_specs=[hbm, vmem, vmem, vmem] + [hbm] * 7,
            out_specs=(hbm, hbm),
            scratch_shapes=[
                pltpu.VMEM((2 * n_tok, width), BF16),
                pltpu.VMEM((2 * n_tok, 3 * half), BF16),
                pltpu.VMEM((2 * n_tok, half), BF16),
                pltpu.VMEM((n_tok, half), BF16),
                pltpu.VMEM((n_tok, width), BF16),
                pltpu.VMEM((2 * n_tok, width), BF16),
                pltpu.VMEM((2 * n_tok, ff // 2), BF16),
                pltpu.VMEM((n_tok, width), F32),
                pltpu.VMEM((n_tok, width), F32),
                pltpu.VMEM((n_tok, width), F32),
                pltpu.VMEM((2, n_fsdp, rows, SLAB), BF16),
                pltpu.VMEM((2 * n_tok, 128), F32),
                pltpu.VMEM((2 * n_tok, 128), F32),
                pltpu.VMEM((4 * n_layers, width), F32),
                pltpu.SemaphoreType.DMA((n_stage,)),
                pltpu.SemaphoreType.DMA((n_stage,)),
                pltpu.SemaphoreType.DMA((n_stage,)),
                pltpu.SemaphoreType.DMA((n_stage,)),
                pltpu.SemaphoreType.DMA((2,)),
                pltpu.SemaphoreType.DMA((2,)),
                pltpu.SemaphoreType.DMA((10,)),
                pltpu.SemaphoreType.DMA((2, width // 512)),
                pltpu.SemaphoreType.DMA((2,)),
            ],
            compiler_params=pltpu.CompilerParams(collective_id=0, has_side_effects=True, vmem_limit_bytes=62 * 1024 * 1024),
        )(tokens.reshape(n_tok, width), gains, jnp.asarray(cos_tab), jnp.asarray(sin_tab), w_query, w_key, w_value, w_out, w_gate, w_up, w_down)
        return result.reshape(n_seq, seq_len, width)

    mapped = jax.shard_map(local_fn, mesh=mesh, in_specs=(P(('dp', 'fsdp')), P(None, 'fsdp')), out_specs=P(('dp', 'fsdp')), check_vma=False)

    def run(tokens, w_query, w_key, w_value, w_out, w_gate, w_up, w_down, g_query, g_key, g_attn, g_mlp):
        return mapped(tokens, (w_query, w_key, w_value, w_out, w_gate, w_up, w_down, g_query, g_key, g_attn, g_mlp))

    return run
```

```python
import functools

import jax
import jax.numpy as jnp
import numpy as np
from jax import lax
from jax.experimental import pallas as pl
from jax.experimental.pallas import tpu as pltpu
from jax.sharding import PartitionSpec as P

HEAD_DIM = 128
EPS = 1e-6
THETA = 500000.0
SLAB = 1024
AHEAD = 3
TIGHT = 10
F32 = jnp.float32
BF16 = jnp.bfloat16


def rope_tables(seq_len):
    positions = np.arange(seq_len, dtype=np.float32)
    inv_freq = np.power(np.float32(THETA), -2.0 * np.arange(HEAD_DIM // 2, dtype=np.float32) / np.float32(HEAD_DIM)).astype(np.float32)
    angles = positions[:, None] * inv_freq[None, :]
    cos, sin = np.cos(angles), np.sin(angles)
    return np.concatenate([cos, cos], axis=1), np.concatenate([-sin, sin], axis=1)


def dot(left, right):
    return jnp.dot(left, right, preferred_element_type=F32)


def kernel(dims, tokens, gains, cos_ref, sin_ref, wq, wk, wv, wo, wg, wu, wd, out, gat,
           x2, qkv, att, att_in, alin, h2, mid, p_own, p_out, p_in, wbuf, stat, stat_in, gvec,
           sem_a, sem_b, sem_c, sem_s, sem_w, sem_g, sem_y, sem_p, sem_o, sem_l):
    n, n_layers, n_tok, seq_len, width, rows, ff_blk, d_rows = dims
    half = width // 2
    n_heads = half // HEAD_DIM
    n_qkv, n_out, n_gu, n_down = 3, width // SLAB, n, width // 512
    per_layer = n_qkv + n_out + n_gu + n_down
    n_stage = per_layer * n_layers
    first_out, first_gu, first_down = n_qkv, n_qkv + n_out, n_qkv + n_out + n_gu
    me = lax.axis_index('fsdp')
    group = lax.axis_index('dp')
    part = lax.rem(group, 2)
    pair = {'dp': group + 1 - 2 * part}
    left = lax.rem(me + n - 2, n)
    right = lax.rem(me + 2, n)
    far = lax.rem(me + 4, n)
    sib = me + 1 - 2 * lax.rem(me, 2)
    own_rows = pl.ds(0, n_tok)
    pair_rows = pl.ds(n_tok, n_tok)

    def send(src, dst, s_sem, r_sem, dev):
        copy = pltpu.make_async_remote_copy(src_ref=src, dst_ref=dst, send_sem=s_sem, recv_sem=r_sem, device_id=dev,
                                            device_id_type=pl.DeviceIdType.MESH)
        copy.start()
        return copy

    def arrive(ref, sem):
        pltpu.make_async_copy(ref, ref, sem).wait()

    twin = first_out + 1

    def out_block(layer, i):
        first = 1 - (layer + n_layers - 1) // n_layers
        return lax.rem(i + part * first, 2)

    def own_blocks(layer, pos, do):
        for i, w in enumerate((wq, wk, wv)):
            @pl.when(pos == i)
            def _(w=w):
                do(w.at[layer, :, pl.ds(pl.multiple_of(part * half, 128), half)], slice(0, SLAB))

        @pl.when(jnp.logical_and(pos >= first_out, pos < first_gu))
        def _():
            do(wo.at[layer, :, pl.ds(pl.multiple_of(out_block(layer, pos - first_out) * SLAB, 128), SLAB)], slice(0, SLAB))

        @pl.when(jnp.logical_and(pos >= first_gu, pos < first_down))
        def _():
            cols = pl.ds(pl.multiple_of((pos - first_gu) * 2 * ff_blk + part * ff_blk, 128), ff_blk)
            do(wg.at[layer, :, cols], slice(0, ff_blk))
            do(wu.at[layer, :, cols], slice(ff_blk, 2 * ff_blk))

        @pl.when(pos >= first_down)
        def _():
            cols = pl.ds(pl.multiple_of((pos - first_down) * 512, 128), 512)
            for k in range(2):
                do(wd.at[layer, pl.ds(pl.multiple_of(part * d_rows + k * rows, 128), rows), cols], slice(k * 512, (k + 1) * 512))

    def start_own(s):
        def do(src, cols):
            dst = gat.at[s, me, :, cols]

            @pl.when(jnp.logical_or(s < twin, s > twin))
            def _():
                send(src, dst, sem_s.at[s], sem_a.at[s], {'fsdp': right})
                send(src, dst, sem_s.at[s], sem_a.at[s], {'fsdp': left})
            send(src, dst, sem_s.at[s], sem_c.at[s], {'fsdp': sib})
        own_blocks(s // per_layer, lax.rem(s, per_layer), do)

    def to_twin(origin):
        send(gat.at[twin - 1, origin], gat.at[twin, origin], sem_s.at[twin], sem_b.at[twin], pair)

    def twin_relay():
        arrive(gat.at[twin, pl.ds(0, 3)], sem_b.at[twin])
        for origin in (left, right, far):
            block = gat.at[twin, origin]
            send(block, block, sem_s.at[twin], sem_c.at[twin], {'fsdp': sib})

    def pump(s):
        @pl.when(jnp.logical_and(s < n_stage, jnp.logical_or(s < twin, s > twin)))
        def _():
            arrive(gat.at[s, pl.ds(0, 2)], sem_a.at[s])
            top, bottom = pl.ds(0, rows // 2), pl.ds(rows // 2, rows // 2)
            block = gat.at[s, left, top]
            send(block, block, sem_s.at[s], sem_b.at[s], {'fsdp': right})
            block = gat.at[s, right, bottom]
            send(block, block, sem_s.at[s], sem_b.at[s], {'fsdp': left})
            for origin in (left, right):
                block = gat.at[s, origin]
                send(block, block, sem_s.at[s], sem_c.at[s], {'fsdp': sib})

        @pl.when(s == twin - 1)
        def _():
            for origin in (left, right):
                to_twin(origin)

        pos = lax.rem(s, per_layer)
        wrap = jnp.logical_and(pos == 0, s > 0)

        def own(k, c):
            t = s + AHEAD - 1 + k

            @pl.when(jnp.logical_and(t < n_stage, jnp.logical_or(jnp.logical_and(k == 0, jnp.logical_or(pos > TIGHT, wrap)),
                                                                 jnp.logical_and(k == 1, pos < TIGHT))))
            def _():
                start_own(t)
            return c
        lax.fori_loop(0, 2, own, 0)

        def far_block(k, c):
            t = s - 2 + k
            two = jnp.logical_and(jnp.logical_and(s >= 2, s < n_stage), jnp.logical_and(pos <= TIGHT, jnp.logical_or(pos > 1, s < per_layer)))
            one = jnp.logical_and(s <= n_stage, jnp.logical_or(pos >= TIGHT, wrap))

            @pl.when(jnp.logical_or(jnp.logical_and(k == 0, two), jnp.logical_and(k == 1, one)))
            def _():
                @pl.when(jnp.logical_or(t < twin, t > twin))
                def _():
                    block = gat.at[t, far]
                    arrive(block, sem_b.at[t])
                    send(block, block, sem_s.at[t], sem_c.at[t], {'fsdp': sib})

                @pl.when(t == twin - 1)
                def _():
                    to_twin(far)
            return c
        lax.fori_loop(0, 2, far_block, 0)

    def stage_ready(s):
        arrive(gat.at[s, pl.ds(0, 4)], sem_c.at[s])

    def load(layer, pos, slot):
        s = layer * per_layer + pos
        for k in range(1, n):
            d = lax.rem(me + k, n)
            pltpu.make_async_copy(gat.at[s, d], wbuf.at[slot, d], sem_w.at[slot]).start()
        own_blocks(layer, pos, lambda src, cols: pltpu.make_async_copy(src, wbuf.at[slot, me, :, cols], sem_w.at[slot]).start())

    def loaded(slot):
        arrive(wbuf.at[slot], sem_w.at[slot])

    def tiles(layer, first, count, repeat, compute, pumps):
        stage, fresh = repeat

        def fetch(it):
            pos = first + stage(it)

            @pl.when(fresh(it))
            def _():
                stage_ready(layer * per_layer + pos)
            load(layer, pos, lax.rem(it, 2))

        def body(step, carry):
            @pl.when(step < count)
            def _():
                pumps(step)
                fetch(step)

            @pl.when(step > 0)
            def _():
                slot = lax.rem(step + 1, 2)
                loaded(slot)
                compute(step - 1, slot)
            return carry
        lax.fori_loop(0, count + 1, body, 0)

    def weight(slot, cols):
        return wbuf[slot, :, :, cols].reshape(n * rows, cols.stop - cols.start)

    barrier = pltpu.get_barrier_semaphore()
    for k in range(1, n):
        pl.semaphore_signal(barrier, inc=1, device_id={'fsdp': lax.rem(me + k, n)}, device_id_type=pl.DeviceIdType.MESH)
    pl.semaphore_signal(barrier, inc=1, device_id=pair, device_id_type=pl.DeviceIdType.MESH)
    pl.semaphore_wait(barrier, n)

    def first_own(s, c):
        start_own(s)
        return c
    lax.fori_loop(0, AHEAD, first_own, 0)
    x_copy = send(tokens, x2.at[pair_rows], sem_y.at[0], sem_y.at[1], pair)
    my_gain = gvec.at[:, pl.ds(pl.multiple_of(me * rows, 128), rows)]
    gain_copies = [send(gains, my_gain, sem_g.at[0], sem_g.at[1], {'fsdp': lax.rem(me + k, n)}) for k in range(1, n)]
    local = [pltpu.make_async_copy(tokens, x2.at[own_rows], sem_l.at[0]), pltpu.make_async_copy(gains, my_gain, sem_l.at[1])]
    for c in local:
        c.start()
    for c in local:
        c.wait()
    gain_ref = gvec.at[:, pl.ds(0, (n - 1) * rows)]
    arrive(gain_ref, sem_g.at[0])
    arrive(gain_ref, sem_g.at[1])

    def first_pump(s, c):
        pump(s)
        return c
    lax.fori_loop(0, 3, first_pump, 0)
    x_copy.wait_send()

    blk = 64

    def pick_gain(row, cols):
        table = gvec[:, cols]
        chosen = lax.broadcasted_iota(jnp.int32, table.shape, 0) == row
        return jnp.sum(jnp.where(chosen, table, 0.0), axis=0, keepdims=True)

    def residual_norm(res, lin, dst, gain_row):
        gain = pick_gain(gain_row, slice(None))

        def body(i, carry):
            r = pl.ds(pl.multiple_of(i * blk, blk), blk)
            v = lin(r)
            inv = lax.rsqrt(jnp.mean(v * v, axis=-1, keepdims=True) + EPS)
            dst[r, :] = (res[r, :].astype(F32) + v * inv * gain).astype(BF16)
            return carry
        lax.fori_loop(0, n_tok // blk, body, 0)

    def layer_body(layer, carry):
        base = layer * per_layer

        def pump_span(lo, hi):
            lo, hi = (jnp.where(layer == 0, *v) if isinstance(v, tuple) else v for v in (lo, hi))

            def one(s, c):
                pump(base + s)
                return c
            lax.fori_loop(lo, hi, one, 0)

        def qkv_compute(it, slot):
            @pl.when(it == n_qkv)
            def _():
                pump_span(5, (5, 7))
                arrive(x2.at[pair_rows], sem_y.at[1])
            kind = lax.rem(it, n_qkv)
            r = pl.ds(pl.multiple_of((it // n_qkv) * n_tok, n_tok), n_tok)
            for k in range(SLAB // 512):
                val = dot(x2[r, :], weight(slot, slice(k * 512, (k + 1) * 512))).astype(BF16)
                qkv[r, pl.ds(pl.multiple_of(kind * half + k * 512, 128), 512)] = val
                sq = val.astype(F32)
                ssq = jnp.sum(sq * sq, axis=-1, keepdims=True)
                if k == 0:
                    total = ssq
                else:
                    total = total + ssq
            lane = lax.broadcasted_iota(jnp.int32, (n_tok, 128), 1)
            spread = jnp.broadcast_to(total, (n_tok, 128))

            @pl.when(kind == 0)
            def _():
                stat[r, :] = spread

            @pl.when(kind == 1)
            def _():
                stat[r, :] = jnp.where(lane < 64, stat[r, :], spread)

        def qkv_pumps(it):
            @pl.when(jnp.logical_and(it > 0, it < n_qkv))
            def _():
                pump_span((2 + it, 4), 3 + it)
        tiles(layer, 0, 2 * n_qkv, (lambda it: lax.rem(it, n_qkv), lambda it: it < n_qkv), qkv_compute, qkv_pumps)

        copies = [send(stat.at[own_rows], stat_in.at[pair_rows], sem_y.at[2], sem_y.at[3], pair),
                  send(stat.at[pair_rows], stat_in.at[own_rows], sem_y.at[4], sem_y.at[5], pair)]
        pump_span((5, 7), (6, 8))
        for c in copies:
            c.wait()

        n_seq = n_tok // seq_len

        def attend(it, carry):
            seq = lax.rem(it + n_seq, 2 * n_seq)
            r = pl.ds(pl.multiple_of(seq * seq_len, seq_len), seq_len)
            sums = (stat[r, :] + stat_in[r, :]) * (1.0 / width)
            inv = lax.rsqrt(sums + EPS)
            inv_q, inv_k = inv[:, 0:1], inv[:, 64:65]
            causal = lax.broadcasted_iota(jnp.int32, (seq_len, seq_len), 0) >= lax.broadcasted_iota(jnp.int32, (seq_len, seq_len), 1)

            def norm_rope(vals, inv_rms, gain):
                v = vals.astype(F32) * inv_rms * gain
                return (v * cos_ref[...] + pltpu.roll(v, HEAD_DIM // 2, 1) * sin_ref[...]).astype(BF16)

            def head(h, c2):
                col = pl.multiple_of(h * HEAD_DIM, HEAD_DIM)
                gcol = pl.ds(pl.multiple_of(part * half + col, HEAD_DIM), HEAD_DIM)
                q = norm_rope(qkv[r, pl.ds(col, HEAD_DIM)], inv_q, pick_gain(layer, gcol))
                k = norm_rope(qkv[r, pl.ds(pl.multiple_of(half + col, HEAD_DIM), HEAD_DIM)], inv_k, pick_gain(n_layers + layer, gcol))
                v = qkv[r, pl.ds(pl.multiple_of(2 * half + col, HEAD_DIM), HEAD_DIM)]
                sc = lax.dot_general(q, k, (((1,), (1,)), ((), ())), preferred_element_type=F32) * HEAD_DIM ** -0.5
                sc = jnp.where(causal, sc, -jnp.inf)
                e = jnp.exp(sc - jnp.max(sc, axis=-1, keepdims=True))
                p = (e / jnp.sum(e, axis=-1, keepdims=True)).astype(BF16)
                att[r, pl.ds(col, HEAD_DIM)] = dot(p, v).astype(BF16)
                return c2
            lax.fori_loop(0, n_heads, head, 0)


            @pl.when(it < n_seq)
            def _():
                send(att.at[r], att_in.at[pl.ds(pl.multiple_of(it * seq_len, seq_len), seq_len)], sem_o.at[0, it], sem_o.at[1, it], pair)

            @pl.when(lax.rem(it, 2) == 1)
            def _():
                pump_span((6 + it // 2, 8 + it // 2), (7, 9 + it // 2))
            return carry
        lax.fori_loop(0, 2 * n_seq, attend, 0)
        for i in range(n_seq):
            for k in range(2):
                arrive(att_in.at[pl.ds(i * seq_len, seq_len)], sem_o.at[k, i])

        @pl.when(layer == 0)
        def _():
            twin_relay()
        def out_compute(it, slot):
            q = n // 2
            for k in range(SLAB // 512):
                cols = slice(k * 512, (k + 1) * 512)
                w_mine = wbuf[slot, pl.ds(part * q, q), :, cols].reshape(q * rows, 512)
                w_theirs = wbuf[slot, pl.ds((1 - part) * q, q), :, cols].reshape(q * rows, 512)
                val = dot(att[own_rows, :], w_mine) + dot(att_in[...], w_theirs)
                alin[:, pl.ds(pl.multiple_of(out_block(layer, it) * SLAB + k * 512, 128), 512)] = val.astype(BF16)

        def out_pumps(it):
            return
        tiles(layer, first_out, n_out, (lambda it: it, lambda it: it >= 0), out_compute, out_pumps)
        residual_norm(x2, lambda r: alin[r, :].astype(F32), h2, 2 * n_layers + layer)
        h_copy = send(h2.at[own_rows], h2.at[pair_rows], sem_y.at[8], sem_y.at[9], pair)
        pump_span((7, 10), (7, 11))

        n_early = n_gu - 2

        def gu_compute(d, theirs, slot):
            r = pl.ds(pl.multiple_of(theirs * n_tok, n_tok), n_tok)
            for k in range(2):
                w = ff_blk // 2
                g = dot(h2[r, :], weight(slot, slice(k * w, (k + 1) * w))).astype(BF16).astype(F32)
                u = dot(h2[r, :], weight(slot, slice(ff_blk + k * w, ff_blk + (k + 1) * w))).astype(BF16).astype(F32)
                mid[r, pl.ds(pl.multiple_of(k * n * rows + d * w, 128), w)] = (jax.nn.silu(g) * u).astype(BF16)

        def gu_early(it, slot):
            @pl.when(it == n_early)
            def _():
                h_copy.wait()
            gu_compute(lax.rem(it, n_early), it // n_early, slot)

        def early_pumps(it):
            @pl.when(it < 4)
            def _():
                pump_span((7 + it, 11), (8 + it, 11))

            @pl.when(jnp.logical_or(it == 5, it == 6))
            def _():
                pump_span(6 + it, (12, 7 + it))
        tiles(layer, first_gu, 2 * n_early, (lambda it: lax.rem(it, n_early), lambda it: it < n_early), gu_early, early_pumps)

        def late_pumps(it):
            @pl.when(lax.rem(it, 2) == 0)
            def _():
                pump_span((12 + it // 2, 13), 13 + it // 2)
        tiles(layer, first_gu + n_early, 2 * (n_gu - n_early), (lambda it: it // 2, lambda it: lax.rem(it, 2) == 0),
              lambda it, slot: gu_compute(n_early + it // 2, lax.rem(it, 2), slot), late_pumps)

        def down_compute(it, slot):
            c = it // 2
            cols = pl.ds(pl.multiple_of(c * 512, 512), 512)
            mine = lax.rem(it, 2)
            r = pl.ds(pl.multiple_of((1 - mine) * n_tok, n_tok), n_tok)
            k_half = n * rows
            val = dot(mid[r, 0:k_half], weight(slot, slice(0, 512))) + dot(mid[r, k_half:2 * k_half], weight(slot, slice(512, 1024)))

            @pl.when(mine == 1)
            def _():
                p_own[:, cols] = val

            @pl.when(mine == 0)
            def _():
                p_out[:, cols] = val
                send(p_out.at[:, cols], p_in.at[:, cols], sem_p.at[0, c], sem_p.at[1, c], pair)

        def down_pumps(it):
            @pl.when(lax.rem(it, 2) == 0)
            def _():
                pump_span(14 + it // 2, 15 + it // 2)
        tiles(layer, first_down, 2 * n_down, (lambda it: it // 2, lambda it: lax.rem(it, 2) == 0), down_compute, down_pumps)
        pump_span(18, 21)
        for c in range(n_down):
            for k in range(2):
                arrive(p_in.at[:, pl.ds(c * 512, 512)], sem_p.at[k, c])
        @pl.when(layer > 0)
        def _():
            arrive(x2.at[own_rows], sem_y.at[0])
        residual_norm(h2, lambda r: (p_own[r, :] + p_in[r, :]).astype(BF16).astype(F32), x2, 3 * n_layers + layer)

        @pl.when(layer + 1 < n_layers)
        def _():
            send(x2.at[own_rows], x2.at[pair_rows], sem_y.at[0], sem_y.at[1], pair)
        return carry
    lax.fori_loop(0, n_layers, layer_body, 0)

    done = pltpu.make_async_copy(x2.at[own_rows], out, sem_l.at[0])
    done.start()
    done.wait()

    def drain(s, carry):
        arrive(gat.at[s, pl.ds(0, 7)], sem_s.at[s])
        return carry
    lax.fori_loop(0, n_stage, drain, 0)


def solution(mesh):
    n_fsdp = mesh.shape['fsdp']

    def local_fn(tokens, weights):
        w_query, w_key, w_value, w_out, w_gate, w_up, w_down, g_query, g_key, g_attn, g_mlp = weights
        n_layers, rows, width = w_query.shape
        n_seq, seq_len, _ = tokens.shape
        n_tok = n_seq * seq_len
        ff = w_gate.shape[2]
        half = width // 2
        ff_blk = ff // n_fsdp // 2
        d_rows = w_down.shape[1] // 2
        dims = (n_fsdp, n_layers, n_tok, seq_len, width, rows, ff_blk, d_rows)
        n_stage = n_layers * (3 + width // SLAB + n_fsdp + width // 512)
        gains = jnp.concatenate([g_query, g_key, g_attn, g_mlp], axis=0).astype(F32)
        cos_tab, sin_tab = rope_tables(seq_len)
        hbm = pl.BlockSpec(memory_space=pl.ANY)
        vmem = pl.BlockSpec(memory_space=pltpu.VMEM)
        result, _ = pl.pallas_call(
            functools.partial(kernel, dims),
            out_shape=(jax.ShapeDtypeStruct((n_tok, width), BF16), jax.ShapeDtypeStruct((n_stage, n_fsdp, rows, SLAB), BF16)),
            in_specs=[hbm, vmem, vmem, vmem] + [hbm] * 7,
            out_specs=(hbm, hbm),
            scratch_shapes=[
                pltpu.VMEM((2 * n_tok, width), BF16),
                pltpu.VMEM((2 * n_tok, 3 * half), BF16),
                pltpu.VMEM((2 * n_tok, half), BF16),
                pltpu.VMEM((n_tok, half), BF16),
                pltpu.VMEM((n_tok, width), BF16),
                pltpu.VMEM((2 * n_tok, width), BF16),
                pltpu.VMEM((2 * n_tok, ff // 2), BF16),
                pltpu.VMEM((n_tok, width), F32),
                pltpu.VMEM((n_tok, width), F32),
                pltpu.VMEM((n_tok, width), F32),
                pltpu.VMEM((2, n_fsdp, rows, SLAB), BF16),
                pltpu.VMEM((2 * n_tok, 128), F32),
                pltpu.VMEM((2 * n_tok, 128), F32),
                pltpu.VMEM((4 * n_layers, width), F32),
                pltpu.SemaphoreType.DMA((n_stage,)),
                pltpu.SemaphoreType.DMA((n_stage,)),
                pltpu.SemaphoreType.DMA((n_stage,)),
                pltpu.SemaphoreType.DMA((n_stage,)),
                pltpu.SemaphoreType.DMA((2,)),
                pltpu.SemaphoreType.DMA((2,)),
                pltpu.SemaphoreType.DMA((10,)),
                pltpu.SemaphoreType.DMA((2, width // 512)),
                pltpu.SemaphoreType.DMA((2, n_seq)),
                pltpu.SemaphoreType.DMA((2,)),
            ],
            compiler_params=pltpu.CompilerParams(collective_id=0, has_side_effects=True, vmem_limit_bytes=62 * 1024 * 1024),
        )(tokens.reshape(n_tok, width), gains, jnp.asarray(cos_tab), jnp.asarray(sin_tab), w_query, w_key, w_value, w_out, w_gate, w_up, w_down)
        return result.reshape(n_seq, seq_len, width)

    mapped = jax.shard_map(local_fn, mesh=mesh, in_specs=(P(('dp', 'fsdp')), P(None, 'fsdp')), out_specs=P(('dp', 'fsdp')), check_vma=False)

    def run(tokens, w_query, w_key, w_value, w_out, w_gate, w_up, w_down, g_query, g_key, g_attn, g_mlp):
        return mapped(tokens, (w_query, w_key, w_value, w_out, w_gate, w_up, w_down, g_query, g_key, g_attn, g_mlp))

    return run
```

```python
import functools

import jax
import jax.numpy as jnp
import numpy as np
from jax import lax
from jax.experimental import pallas as pl
from jax.experimental.pallas import tpu as pltpu
from jax.sharding import PartitionSpec as P

HEAD_DIM = 128
EPS = 1e-6
THETA = 500000.0
SLAB = 1024
AHEAD = 3
TIGHT = 10
F32 = jnp.float32
BF16 = jnp.bfloat16


def rope_tables(seq_len):
    positions = np.arange(seq_len, dtype=np.float32)
    inv_freq = np.power(np.float32(THETA), -2.0 * np.arange(HEAD_DIM // 2, dtype=np.float32) / np.float32(HEAD_DIM)).astype(np.float32)
    angles = positions[:, None] * inv_freq[None, :]
    cos, sin = np.cos(angles), np.sin(angles)
    return np.concatenate([cos, cos], axis=1), np.concatenate([-sin, sin], axis=1)


def dot(left, right):
    return jnp.dot(left, right, preferred_element_type=F32)


def kernel(dims, tokens, gains, cos_ref, sin_ref, wq, wk, wv, wo, wg, wu, wd, out, gat,
           x2, qkv, att, att_in, alin, h2, mid, p_own, p_out, p_in, wbuf, stat, stat_in, gvec,
           sem_a, sem_b, sem_c, sem_s, sem_w, sem_g, sem_y, sem_p, sem_o, sem_l):
    n, n_layers, n_tok, seq_len, width, rows, ff_blk, d_rows = dims
    half = width // 2
    n_heads = half // HEAD_DIM
    n_qkv, n_out, n_gu, n_down = 3, width // SLAB, n, width // 512
    per_layer = n_qkv + n_out + n_gu + n_down
    n_stage = per_layer * n_layers
    first_out, first_gu, first_down = n_qkv, n_qkv + n_out, n_qkv + n_out + n_gu
    me = lax.axis_index('fsdp')
    group = lax.axis_index('dp')
    part = lax.rem(group, 2)
    pair = {'dp': group + 1 - 2 * part}
    left = lax.rem(me + n - 2, n)
    right = lax.rem(me + 2, n)
    far = lax.rem(me + 4, n)
    sib = me + 1 - 2 * lax.rem(me, 2)
    own_rows = pl.ds(0, n_tok)
    pair_rows = pl.ds(n_tok, n_tok)

    def send(src, dst, s_sem, r_sem, dev):
        copy = pltpu.make_async_remote_copy(src_ref=src, dst_ref=dst, send_sem=s_sem, recv_sem=r_sem, device_id=dev,
                                            device_id_type=pl.DeviceIdType.MESH)
        copy.start()
        return copy

    def arrive(ref, sem):
        pltpu.make_async_copy(ref, ref, sem).wait()

    twin = first_out + 1

    def out_block(layer, i):
        first = 1 - (layer + n_layers - 1) // n_layers
        return lax.rem(i + part * first, 2)

    def own_blocks(layer, pos, do):
        for i, w in enumerate((wq, wk, wv)):
            @pl.when(pos == i)
            def _(w=w):
                do(w.at[layer, :, pl.ds(pl.multiple_of(part * half, 128), half)], slice(0, SLAB))

        @pl.when(jnp.logical_and(pos >= first_out, pos < first_gu))
        def _():
            do(wo.at[layer, :, pl.ds(pl.multiple_of(out_block(layer, pos - first_out) * SLAB, 128), SLAB)], slice(0, SLAB))

        @pl.when(jnp.logical_and(pos >= first_gu, pos < first_down))
        def _():
            cols = pl.ds(pl.multiple_of((pos - first_gu) * 2 * ff_blk + part * ff_blk, 128), ff_blk)
            do(wg.at[layer, :, cols], slice(0, ff_blk))
            do(wu.at[layer, :, cols], slice(ff_blk, 2 * ff_blk))

        @pl.when(pos >= first_down)
        def _():
            cols = pl.ds(pl.multiple_of((pos - first_down) * 512, 128), 512)
            for k in range(2):
                do(wd.at[layer, pl.ds(pl.multiple_of(part * d_rows + k * rows, 128), rows), cols], slice(k * 512, (k + 1) * 512))

    def start_own(s):
        def do(src, cols):
            dst = gat.at[s, me, :, cols]

            @pl.when(jnp.logical_or(s < twin, s > twin))
            def _():
                send(src, dst, sem_s.at[s], sem_a.at[s], {'fsdp': right})
                send(src, dst, sem_s.at[s], sem_a.at[s], {'fsdp': left})
            send(src, dst, sem_s.at[s], sem_c.at[s], {'fsdp': sib})
        own_blocks(s // per_layer, lax.rem(s, per_layer), do)

    def to_twin(origin):
        send(gat.at[twin - 1, origin], gat.at[twin, origin], sem_s.at[twin], sem_b.at[twin], pair)

    def twin_relay():
        arrive(gat.at[twin, pl.ds(0, 3)], sem_b.at[twin])
        for origin in (left, right, far):
            block = gat.at[twin, origin]
            send(block, block, sem_s.at[twin], sem_c.at[twin], {'fsdp': sib})

    def pump(s):
        @pl.when(jnp.logical_and(s < n_stage, jnp.logical_or(s < twin, s > twin)))
        def _():
            arrive(gat.at[s, pl.ds(0, 2)], sem_a.at[s])
            top, bottom = pl.ds(0, rows // 2), pl.ds(rows // 2, rows // 2)
            block = gat.at[s, left, top]
            send(block, block, sem_s.at[s], sem_b.at[s], {'fsdp': right})
            block = gat.at[s, right, bottom]
            send(block, block, sem_s.at[s], sem_b.at[s], {'fsdp': left})
            for origin in (left, right):
                block = gat.at[s, origin]
                send(block, block, sem_s.at[s], sem_c.at[s], {'fsdp': sib})

        @pl.when(s == twin - 1)
        def _():
            for origin in (left, right):
                to_twin(origin)

        pos = lax.rem(s, per_layer)
        wrap = jnp.logical_and(pos == 0, s > 0)

        def own(k, c):
            t = s + AHEAD - 1 + k

            @pl.when(jnp.logical_and(t < n_stage, jnp.logical_or(jnp.logical_and(k == 0, jnp.logical_or(pos > TIGHT, wrap)),
                                                                 jnp.logical_and(k == 1, pos < TIGHT))))
            def _():
                start_own(t)
            return c
        lax.fori_loop(0, 2, own, 0)

        def far_block(k, c):
            t = s - 2 + k
            two = jnp.logical_and(jnp.logical_and(s >= 2, s < n_stage), jnp.logical_and(pos <= TIGHT, jnp.logical_or(pos > 1, s < per_layer)))
            one = jnp.logical_and(s <= n_stage, jnp.logical_or(pos >= TIGHT, wrap))

            @pl.when(jnp.logical_or(jnp.logical_and(k == 0, two), jnp.logical_and(k == 1, one)))
            def _():
                @pl.when(jnp.logical_or(t < twin, t > twin))
                def _():
                    block = gat.at[t, far]
                    arrive(block, sem_b.at[t])
                    send(block, block, sem_s.at[t], sem_c.at[t], {'fsdp': sib})

                @pl.when(t == twin - 1)
                def _():
                    to_twin(far)
            return c
        lax.fori_loop(0, 2, far_block, 0)

    def stage_ready(s):
        arrive(gat.at[s, pl.ds(0, 4)], sem_c.at[s])

    def load(layer, pos, slot):
        s = layer * per_layer + pos
        for k in range(1, n):
            d = lax.rem(me + k, n)
            pltpu.make_async_copy(gat.at[s, d], wbuf.at[slot, d], sem_w.at[slot]).start()
        own_blocks(layer, pos, lambda src, cols: pltpu.make_async_copy(src, wbuf.at[slot, me, :, cols], sem_w.at[slot]).start())

    def loaded(slot):
        arrive(wbuf.at[slot], sem_w.at[slot])

    def tiles(layer, first, count, repeat, compute, pumps, paced=False):
        stage, fresh = repeat

        def fetch(it):
            pos = first + stage(it)

            @pl.when(fresh(it))
            def _():
                stage_ready(layer * per_layer + pos)
            load(layer, pos, lax.rem(it, 2))

        def body(step, carry):
            def ahead():
                @pl.when(step < count)
                def _():
                    pumps(step)
                    fetch(step)

            if not paced:
                ahead()

            @pl.when(step > 0)
            def _():
                slot = lax.rem(step + 1, 2)
                loaded(slot)
                compute(step - 1, slot)

            if paced:
                ahead()
            return carry
        lax.fori_loop(0, count + 1, body, 0)

    def weight(slot, cols):
        return wbuf[slot, :, :, cols].reshape(n * rows, cols.stop - cols.start)

    barrier = pltpu.get_barrier_semaphore()
    for k in range(1, n):
        pl.semaphore_signal(barrier, inc=1, device_id={'fsdp': lax.rem(me + k, n)}, device_id_type=pl.DeviceIdType.MESH)
    pl.semaphore_signal(barrier, inc=1, device_id=pair, device_id_type=pl.DeviceIdType.MESH)
    pl.semaphore_wait(barrier, n)

    def first_own(s, c):
        start_own(s)
        return c
    lax.fori_loop(0, AHEAD, first_own, 0)
    x_copy = send(tokens, x2.at[pair_rows], sem_y.at[0], sem_y.at[1], pair)
    my_gain = gvec.at[:, pl.ds(pl.multiple_of(me * rows, 128), rows)]
    gain_copies = [send(gains, my_gain, sem_g.at[0], sem_g.at[1], {'fsdp': lax.rem(me + k, n)}) for k in range(1, n)]
    local = [pltpu.make_async_copy(tokens, x2.at[own_rows], sem_l.at[0]), pltpu.make_async_copy(gains, my_gain, sem_l.at[1])]
    for c in local:
        c.start()
    for c in local:
        c.wait()
    gain_ref = gvec.at[:, pl.ds(0, (n - 1) * rows)]
    arrive(gain_ref, sem_g.at[0])
    arrive(gain_ref, sem_g.at[1])

    def first_pump(s, c):
        pump(s)
        return c
    lax.fori_loop(0, 3, first_pump, 0)
    x_copy.wait_send()

    blk = 64

    def pick_gain(row, cols):
        table = gvec[:, cols]
        chosen = lax.broadcasted_iota(jnp.int32, table.shape, 0) == row
        return jnp.sum(jnp.where(chosen, table, 0.0), axis=0, keepdims=True)

    def residual_norm(res, lin, dst, gain_row):
        gain = pick_gain(gain_row, slice(None))

        def body(i, carry):
            r = pl.ds(pl.multiple_of(i * blk, blk), blk)
            v = lin(r)
            inv = lax.rsqrt(jnp.mean(v * v, axis=-1, keepdims=True) + EPS)
            dst[r, :] = (res[r, :].astype(F32) + v * inv * gain).astype(BF16)
            return carry
        lax.fori_loop(0, n_tok // blk, body, 0)

    def layer_body(layer, carry):
        base = layer * per_layer

        def pump_span(lo, hi):
            lo, hi = (jnp.where(layer == 0, *v) if isinstance(v, tuple) else v for v in (lo, hi))

            def one(s, c):
                pump(base + s)
                return c
            lax.fori_loop(lo, hi, one, 0)

        def qkv_compute(it, slot):
            @pl.when(it == n_qkv)
            def _():
                pump_span(5, (5, 7))
                arrive(x2.at[pair_rows], sem_y.at[1])
            kind = lax.rem(it, n_qkv)
            r = pl.ds(pl.multiple_of((it // n_qkv) * n_tok, n_tok), n_tok)
            for k in range(SLAB // 512):
                val = dot(x2[r, :], weight(slot, slice(k * 512, (k + 1) * 512))).astype(BF16)
                qkv[r, pl.ds(pl.multiple_of(kind * half + k * 512, 128), 512)] = val
                sq = val.astype(F32)
                ssq = jnp.sum(sq * sq, axis=-1, keepdims=True)
                if k == 0:
                    total = ssq
                else:
                    total = total + ssq
            lane = lax.broadcasted_iota(jnp.int32, (n_tok, 128), 1)
            spread = jnp.broadcast_to(total, (n_tok, 128))

            @pl.when(kind == 0)
            def _():
                stat[r, :] = spread

            @pl.when(kind == 1)
            def _():
                stat[r, :] = jnp.where(lane < 64, stat[r, :], spread)

        def qkv_pumps(it):
            @pl.when(jnp.logical_and(it > 0, it < n_qkv))
            def _():
                pump_span((2 + it, 4), 3 + it)
        tiles(layer, 0, 2 * n_qkv, (lambda it: lax.rem(it, n_qkv), lambda it: it < n_qkv), qkv_compute, qkv_pumps)

        copies = [send(stat.at[own_rows], stat_in.at[pair_rows], sem_y.at[2], sem_y.at[3], pair),
                  send(stat.at[pair_rows], stat_in.at[own_rows], sem_y.at[4], sem_y.at[5], pair)]
        pump_span((5, 7), (7, 8))
        for c in copies:
            c.wait()

        n_seq = n_tok // seq_len

        def attend(it, carry):
            seq = lax.rem(it + n_seq, 2 * n_seq)
            r = pl.ds(pl.multiple_of(seq * seq_len, seq_len), seq_len)
            sums = (stat[r, :] + stat_in[r, :]) * (1.0 / width)
            inv = lax.rsqrt(sums + EPS)
            inv_q, inv_k = inv[:, 0:1], inv[:, 64:65]
            causal = lax.broadcasted_iota(jnp.int32, (seq_len, seq_len), 0) >= lax.broadcasted_iota(jnp.int32, (seq_len, seq_len), 1)

            def norm_rope(vals, inv_rms, gain):
                v = vals.astype(F32) * inv_rms * gain
                return (v * cos_ref[...] + pltpu.roll(v, HEAD_DIM // 2, 1) * sin_ref[...]).astype(BF16)

            def head(h, c2):
                col = pl.multiple_of(h * HEAD_DIM, HEAD_DIM)
                gcol = pl.ds(pl.multiple_of(part * half + col, HEAD_DIM), HEAD_DIM)
                q = norm_rope(qkv[r, pl.ds(col, HEAD_DIM)], inv_q, pick_gain(layer, gcol))
                k = norm_rope(qkv[r, pl.ds(pl.multiple_of(half + col, HEAD_DIM), HEAD_DIM)], inv_k, pick_gain(n_layers + layer, gcol))
                v = qkv[r, pl.ds(pl.multiple_of(2 * half + col, HEAD_DIM), HEAD_DIM)]
                sc = lax.dot_general(q, k, (((1,), (1,)), ((), ())), preferred_element_type=F32) * HEAD_DIM ** -0.5
                sc = jnp.where(causal, sc, -jnp.inf)
                e = jnp.exp(sc - jnp.max(sc, axis=-1, keepdims=True))
                p = (e / jnp.sum(e, axis=-1, keepdims=True)).astype(BF16)
                att[r, pl.ds(col, HEAD_DIM)] = dot(p, v).astype(BF16)
                return c2
            lax.fori_loop(0, n_heads, head, 0)


            @pl.when(it < n_seq)
            def _():
                send(att.at[r], att_in.at[pl.ds(pl.multiple_of(it * seq_len, seq_len), seq_len)], sem_o.at[0, it], sem_o.at[1, it], pair)

            @pl.when(lax.rem(it, 2) == 1)
            def _():
                pump_span((7 + it // 2, 8 + it // 2), (8 + it // 2, 9 + it // 2))
            return carry
        lax.fori_loop(0, 2 * n_seq, attend, 0)
        for i in range(n_seq):
            for k in range(2):
                arrive(att_in.at[pl.ds(i * seq_len, seq_len)], sem_o.at[k, i])

        @pl.when(layer == 0)
        def _():
            twin_relay()
        def out_compute(it, slot):
            q = n // 2
            for k in range(SLAB // 512):
                cols = slice(k * 512, (k + 1) * 512)
                w_mine = wbuf[slot, pl.ds(part * q, q), :, cols].reshape(q * rows, 512)
                w_theirs = wbuf[slot, pl.ds((1 - part) * q, q), :, cols].reshape(q * rows, 512)
                val = dot(att[own_rows, :], w_mine) + dot(att_in[...], w_theirs)
                alin[:, pl.ds(pl.multiple_of(out_block(layer, it) * SLAB + k * 512, 128), 512)] = val.astype(BF16)

        def out_pumps(it):
            return
        tiles(layer, first_out, n_out, (lambda it: it, lambda it: it >= 0), out_compute, out_pumps)
        residual_norm(x2, lambda r: alin[r, :].astype(F32), h2, 2 * n_layers + layer)
        h_copy = send(h2.at[own_rows], h2.at[pair_rows], sem_y.at[8], sem_y.at[9], pair)
        pump_span((9, 10), (9, 11))

        n_early = n_gu - 2

        def gu_compute(d, theirs, slot):
            r = pl.ds(pl.multiple_of(theirs * n_tok, n_tok), n_tok)
            for k in range(2):
                w = ff_blk // 2
                g = dot(h2[r, :], weight(slot, slice(k * w, (k + 1) * w))).astype(BF16).astype(F32)
                u = dot(h2[r, :], weight(slot, slice(ff_blk + k * w, ff_blk + (k + 1) * w))).astype(BF16).astype(F32)
                mid[r, pl.ds(pl.multiple_of(k * n * rows + d * w, 128), w)] = (jax.nn.silu(g) * u).astype(BF16)

        def gu_early(it, slot):
            @pl.when(it == n_early)
            def _():
                h_copy.wait()
            gu_compute(lax.rem(it, n_early), it // n_early, slot)

        def early_pumps(it):
            @pl.when(jnp.logical_and(it >= 2, it < 4))
            def _():
                pump_span((7 + it, 9 + it), (8 + it, 12))

            @pl.when(it == 5)
            def _():
                pump_span((11, 12), (12, 13))

            @pl.when(it == 10)
            def _():
                pump_span((12, 13), (12, 14))
        tiles(layer, first_gu, 2 * n_early, (lambda it: lax.rem(it, n_early), lambda it: it < n_early), gu_early, early_pumps)

        def late_pumps(it):
            pump_span((12 + it, 14), (13 + it, 14))
        tiles(layer, first_gu + n_early, n_gu - n_early, (lambda it: it, lambda it: it >= 0),
              lambda it, slot: gu_compute(n_early + it, 1, slot), late_pumps, paced=True)

        def down_dot(c, r, slot):
            k_half = n * rows
            return dot(mid[r, 0:k_half], weight(slot, slice(0, 512))) + dot(mid[r, k_half:2 * k_half], weight(slot, slice(512, 1024)))

        def down_pair(it, slot):
            cols = pl.ds(pl.multiple_of(it * 512, 512), 512)
            p_out[:, cols] = down_dot(it, pair_rows, slot)
            send(p_out.at[:, cols], p_in.at[:, cols], sem_p.at[0, it], sem_p.at[1, it], pair)

        def down_pumps(it):
            pump_span(14 + it, 15 + it)
        tiles(layer, first_down, n_down, (lambda it: it, lambda it: it >= 0), down_pair, down_pumps, paced=True)

        def no_pumps(it):
            pass
        tiles(layer, first_gu + n_early, n_gu - n_early, (lambda it: it, lambda it: it < 0),
              lambda it, slot: gu_compute(n_early + it, 0, slot), no_pumps)

        def down_own(it, slot):
            p_own[:, pl.ds(pl.multiple_of(it * 512, 512), 512)] = down_dot(it, own_rows, slot)
        tiles(layer, first_down, n_down, (lambda it: it, lambda it: it < 0), down_own, no_pumps)
        pump_span(18, 21)
        for c in range(n_down):
            for k in range(2):
                arrive(p_in.at[:, pl.ds(c * 512, 512)], sem_p.at[k, c])
        @pl.when(layer > 0)
        def _():
            arrive(x2.at[own_rows], sem_y.at[0])
        residual_norm(h2, lambda r: (p_own[r, :] + p_in[r, :]).astype(BF16).astype(F32), x2, 3 * n_layers + layer)

        @pl.when(layer + 1 < n_layers)
        def _():
            send(x2.at[own_rows], x2.at[pair_rows], sem_y.at[0], sem_y.at[1], pair)
        return carry
    lax.fori_loop(0, n_layers, layer_body, 0)

    done = pltpu.make_async_copy(x2.at[own_rows], out, sem_l.at[0])
    done.start()
    done.wait()

    def drain(s, carry):
        arrive(gat.at[s, pl.ds(0, 7)], sem_s.at[s])
        return carry
    lax.fori_loop(0, n_stage, drain, 0)


def solution(mesh):
    n_fsdp = mesh.shape['fsdp']

    def local_fn(tokens, weights):
        w_query, w_key, w_value, w_out, w_gate, w_up, w_down, g_query, g_key, g_attn, g_mlp = weights
        n_layers, rows, width = w_query.shape
        n_seq, seq_len, _ = tokens.shape
        n_tok = n_seq * seq_len
        ff = w_gate.shape[2]
        half = width // 2
        ff_blk = ff // n_fsdp // 2
        d_rows = w_down.shape[1] // 2
        dims = (n_fsdp, n_layers, n_tok, seq_len, width, rows, ff_blk, d_rows)
        n_stage = n_layers * (3 + width // SLAB + n_fsdp + width // 512)
        gains = jnp.concatenate([g_query, g_key, g_attn, g_mlp], axis=0).astype(F32)
        cos_tab, sin_tab = rope_tables(seq_len)
        hbm = pl.BlockSpec(memory_space=pl.ANY)
        vmem = pl.BlockSpec(memory_space=pltpu.VMEM)
        result, _ = pl.pallas_call(
            functools.partial(kernel, dims),
            out_shape=(jax.ShapeDtypeStruct((n_tok, width), BF16), jax.ShapeDtypeStruct((n_stage, n_fsdp, rows, SLAB), BF16)),
            in_specs=[hbm, vmem, vmem, vmem] + [hbm] * 7,
            out_specs=(hbm, hbm),
            scratch_shapes=[
                pltpu.VMEM((2 * n_tok, width), BF16),
                pltpu.VMEM((2 * n_tok, 3 * half), BF16),
                pltpu.VMEM((2 * n_tok, half), BF16),
                pltpu.VMEM((n_tok, half), BF16),
                pltpu.VMEM((n_tok, width), BF16),
                pltpu.VMEM((2 * n_tok, width), BF16),
                pltpu.VMEM((2 * n_tok, ff // 2), BF16),
                pltpu.VMEM((n_tok, width), F32),
                pltpu.VMEM((n_tok, width), F32),
                pltpu.VMEM((n_tok, width), F32),
                pltpu.VMEM((2, n_fsdp, rows, SLAB), BF16),
                pltpu.VMEM((2 * n_tok, 128), F32),
                pltpu.VMEM((2 * n_tok, 128), F32),
                pltpu.VMEM((4 * n_layers, width), F32),
                pltpu.SemaphoreType.DMA((n_stage,)),
                pltpu.SemaphoreType.DMA((n_stage,)),
                pltpu.SemaphoreType.DMA((n_stage,)),
                pltpu.SemaphoreType.DMA((n_stage,)),
                pltpu.SemaphoreType.DMA((2,)),
                pltpu.SemaphoreType.DMA((2,)),
                pltpu.SemaphoreType.DMA((10,)),
                pltpu.SemaphoreType.DMA((2, width // 512)),
                pltpu.SemaphoreType.DMA((2, n_seq)),
                pltpu.SemaphoreType.DMA((2,)),
            ],
            compiler_params=pltpu.CompilerParams(collective_id=0, has_side_effects=True, vmem_limit_bytes=62 * 1024 * 1024),
        )(tokens.reshape(n_tok, width), gains, jnp.asarray(cos_tab), jnp.asarray(sin_tab), w_query, w_key, w_value, w_out, w_gate, w_up, w_down)
        return result.reshape(n_seq, seq_len, width)

    mapped = jax.shard_map(local_fn, mesh=mesh, in_specs=(P(('dp', 'fsdp')), P(None, 'fsdp')), out_specs=P(('dp', 'fsdp')), check_vma=False)

    def run(tokens, w_query, w_key, w_value, w_out, w_gate, w_up, w_down, g_query, g_key, g_attn, g_mlp):
        return mapped(tokens, (w_query, w_key, w_value, w_out, w_gate, w_up, w_down, g_query, g_key, g_attn, g_mlp))

    return run
```
